512 devices in a mesh: cuts: 32 (over x, y, core), tr: 16 (over z).
Axes of the slice: x: 4, y: 4, z: 16, core: 2. Of those that a mesh axis runs over, the one named last changes fastest.
Arguments:
- cells: int32 [2, 32, 2, 1024], P(None, 'cuts'), may hold values from 1 to 509
- offsets: float32 [2, 32, 2, 1024], P(None, 'cuts'), may hold values from 0 to 1
- charges: float32 [2, 32, 1024], P(None, 'cuts'), may hold values from 0.5 to 2
- momenta: float32 [2, 32, 2, 1024], P(None, 'cuts', None, 'tr'), may hold values from -6 to 6
- green: float32 [1024, 1024], replicated, may hold values from -0.1875 to 0.1875
Outputs:
- momenta_out: float32 [2, 32, 2, 1024], P(None, 'cuts', None, 'tr')
The draws below stay inside these ranges and needn't reach their ends.
Inputs may be any that keep to these rules, and one draw needn't show every extreme that they name: `cells`: every cell index lies in 1 .. 509.
All inputs are finite; a program needn't handle non-finite values.
Results may differ from the reference program's by a relative error of at most 0.017.
Values may be sent and summed in bfloat16 or wider, within the bound.
A program may use at most 64 MiB of HBM per device.

```python
import math
import jax
import jax.numpy as jnp
from jax import lax

G = 512
NP = 1024
SECTIONS = 4
PAD = 1024
SL = 32


def with_ends(array, own_key, least, high):
    longest = array.shape.index(max(array.shape))
    spots = []
    for shift in (0, 1):
        where = [jax.random.randint(jax.random.fold_in(own_key, axis), (), 0, length) for axis, length in enumerate(array.shape)]
        where[longest] = (where[longest] + shift) % array.shape[longest]
        spots.append(tuple(where))
    return array.at[spots[0]].set(least).at[spots[1]].set(high)


def steps_of(stream_key, dims, split, low, largest):
    factor_of, own = 1.0, jax.random.fold_in(stream_key, 6)
    for dim, blocks in split:
        draws = jnp.exp(jax.random.uniform(jax.random.fold_in(own, dim), (blocks,), jnp.float32, low / len(split), largest / len(split)))
        factor_of = factor_of * jnp.repeat(draws, dims[dim] // blocks).reshape([-1 if axis == dim else 1 for axis in range(len(dims))])
    return factor_of


def gaussian(stream_key, shape, scale, most, cuts=(), kind=jnp.bfloat16):
    result = jax.random.normal(stream_key, shape, jnp.float32) * scale
    if len(cuts) > 0:
        result = steps_of(stream_key, shape, cuts, -0.22, 0.18) * result
    return jnp.clip(result, min=-most, max=most).astype(kind)


def setup_inputs(seed: int = 0) -> dict:
    keys = jax.random.split(jax.random.key(seed), 6)
    return {
        "cells": with_ends(jax.random.randint(keys[0], (2, SL, 2, NP), 1, G - 2), jax.random.fold_in(keys[0], 1), 1, (G - 2) - 1).astype(jnp.int32),
        "offsets": jnp.clip(1.0 * jax.random.uniform(keys[1], (2, SL, 2, NP), jnp.float32) ** steps_of(keys[1], (2, SL, 2, NP), ((1, 32),), -0.2, 0.2), 0.0, 1.0),
        "charges": jnp.clip(jnp.exp(math.log(2.0) - 1.3862944 * jax.random.uniform(keys[2], (2, SL, NP), jnp.float32) ** steps_of(keys[2], (2, SL, NP), ((1, 32),), -0.2, 0.2)), 0.5, 2.0),
        "momenta": gaussian(keys[3], (2, SL, 2, NP), 1.0, 6.0, ((1, 32), (3, 16)), jnp.float32),
        "green": gaussian(keys[4], (PAD, PAD), NP ** -0.5, 0.1875, (), jnp.float32),
    }


drift_step = 0.5


def rounded(values):
    return lax.optimization_barrier(values.astype(jnp.bfloat16)).astype(jnp.float32)


def product(left, right):
    return jnp.dot(left, right, precision=lax.Precision.HIGHEST)


def phase_angles(frequency, position, period):
    return (2.0 * math.pi / period) * ((frequency * position) % period).astype(jnp.float32)


def make_tables(period):
    counter = jnp.arange(period, dtype=jnp.int32)
    theta = phase_angles(counter[:, None], counter[None, :], period)
    return rounded(jnp.cos(theta)), rounded(jnp.sin(theta))


def slice_weights(cells, offsets, charges):
    row_low = rounded(1.0 - offsets[0])
    row_high = rounded(offsets[0])
    col_low = rounded(1.0 - offsets[1])
    col_high = rounded(offsets[1])
    charge_low = rounded(charges * (1.0 - offsets[1]))
    charge_high = rounded(charges * offsets[1])
    return row_low, row_high, col_low, col_high, charge_low, charge_high


def deposit(cells, offsets, charges):
    row_low, row_high, col_low, col_high, charge_low, charge_high = slice_weights(cells, offsets, charges)
    row_cells = cells[0]
    col_cells = cells[1]
    charge_grid = jnp.zeros((G, G), jnp.float32)
    charge_grid = charge_grid.at[row_cells, col_cells].add(row_low * charge_low)
    charge_grid = charge_grid.at[row_cells, col_cells + 1].add(row_low * charge_high)
    charge_grid = charge_grid.at[row_cells + 1, col_cells].add(row_high * charge_low)
    charge_grid = charge_grid.at[row_cells + 1, col_cells + 1].add(row_high * charge_high)
    return rounded(charge_grid)


def potentials(one, two, cosine, sine, kernel_re, kernel_im):
    cos_head = cosine[:G]
    sin_head = sine[:G]
    cos_left = cosine[:, :G]
    sin_left = sine[:, :G]
    first_re = rounded(product(one, cos_head) + product(two, sin_head))
    first_im = rounded(product(two, cos_head) - product(one, sin_head))
    second_re = product(cos_left, first_re) + product(sin_left, first_im)
    second_im = product(cos_left, first_im) - product(sin_left, first_re)
    scaled_re = rounded(second_re * kernel_re - second_im * kernel_im)
    scaled_im = rounded(second_re * kernel_im + second_im * kernel_re)
    back_re = rounded(product(cos_head, scaled_re) - product(sin_head, scaled_im))
    back_im = rounded(product(cos_head, scaled_im) + product(sin_head, scaled_re))
    phi_one = (product(back_re, cos_left) - product(back_im, sin_left)) / (PAD * PAD)
    phi_two = (product(back_im, cos_left) + product(back_re, sin_left)) / (PAD * PAD)
    return phi_one, phi_two


def field_pair(potential):
    widened = jnp.pad(potential, 1)
    along_rows = (widened[:-2, 1:-1] - widened[2:, 1:-1]) * 0.5
    along_cols = (widened[1:-1, :-2] - widened[1:-1, 2:]) * 0.5
    return rounded(along_rows), rounded(along_cols)


def slice_kicks(cells, offsets, field_rows, field_cols):
    row_low, row_high, col_low, col_high, charge_low, charge_high = slice_weights(cells, offsets, offsets[0])
    row_cells = cells[0]
    col_cells = cells[1]

    def sample(field):
        total_low = col_low * field[row_cells, col_cells] + col_high * field[row_cells, col_cells + 1]
        total_high = col_low * field[row_cells + 1, col_cells] + col_high * field[row_cells + 1, col_cells + 1]
        return row_low * total_low + row_high * total_high

    return jnp.stack([sample(field_rows), sample(field_cols)])


def drift(cells, offsets, moment):
    place = cells.astype(jnp.float32) + offsets + drift_step * moment
    place = jnp.clip(place, 1.0, G - 2.0 - 1.0 / 64.0)
    whole = jnp.floor(place)
    return whole.astype(jnp.int32), place - whole


def reference(cells, offsets, charges, momenta, green):
    cosine, sine = make_tables(PAD)
    kernel_grid = rounded(green)
    kernel_cos = rounded(product(kernel_grid, cosine))
    kernel_sin = rounded(-product(kernel_grid, sine))
    kernel_re = product(cosine, kernel_cos) + product(sine, kernel_sin)
    kernel_im = product(cosine, kernel_sin) - product(sine, kernel_cos)
    moment = momenta
    for section_index in range(SECTIONS):
        grids = jax.vmap(jax.vmap(deposit))(cells, offsets, charges)
        visitors = jnp.roll(grids[1], -2 * section_index, axis=0)

        def meeting(inputs):
            phi_one, phi_two = potentials(inputs[0], inputs[1], cosine, sine, kernel_re, kernel_im)
            return field_pair(phi_one), field_pair(phi_two)

        fields_one, fields_two = lax.map(meeting, (grids[0], visitors))
        kick_one = jax.vmap(slice_kicks)(cells[0], offsets[0], fields_two[0], fields_two[1])
        moved_rows = jnp.roll(fields_one[0], 2 * section_index, axis=0)
        moved_cols = jnp.roll(fields_one[1], 2 * section_index, axis=0)
        kick_two = jax.vmap(slice_kicks)(cells[1], offsets[1], moved_rows, moved_cols)
        moment = moment + jnp.stack([kick_one, kick_two])
        if section_index + 1 < SECTIONS:
            cells, offsets = drift(cells, offsets, moment)
    return moment
```

```python
import functools
import math

import jax
import jax.numpy as jnp
import numpy as np
from jax import lax
from jax.experimental import pallas as pl
from jax.experimental.pallas import tpu as pltpu
from jax.sharding import PartitionSpec as P

SECTIONS = 4
GROUP = 4
LANES = 128
DRIFT = 0.5
MESH = pl.DeviceIdType.MESH


def row_tables(period):
    quarter = period // 4
    near = np.arange(quarter)
    forward, backward = [], []
    for residue in range(4):
        angle = 2.0 * np.pi / period * ((near[:, None] * (4 * near[None, :] + residue)) % period)
        forward.append(np.concatenate([np.cos(angle), np.sin(angle)], axis=1))
        backward.append(np.concatenate([np.cos(angle).T, np.sin(angle).T], axis=1))
    return np.stack(forward).astype(jnp.bfloat16), np.stack(backward).astype(jnp.bfloat16)


def column_tables(period):
    extent = period // 2
    count = extent // GROUP
    column = np.arange(extent)
    tables, slopes = [], []
    for rank in range(GROUP):
        twice = 2 * (GROUP * np.arange(count) + rank) + 1
        angle = np.pi / period * ((twice[:, None] * column[None, :]) % (2 * period))
        tables.append(np.concatenate([np.cos(angle), -np.sin(angle)], axis=0))
        slopes.append(np.repeat(np.sin(np.pi / period * twice)[:, None], LANES, axis=1))
    return np.stack(tables).astype(jnp.bfloat16), np.stack(slopes).astype(np.float32)


def dot(left, right):
    return lax.dot_general(left, right, (((1,), (0,)), ((), ())), preferred_element_type=jnp.float32)


def dot_t(left, right):
    return lax.dot_general(left, right, (((1,), (1,)), ((), ())), preferred_element_type=jnp.float32)


def kernel(
    sizes,
    cells_ref, offsets_ref, charges_ref, momenta_ref, green_ref, column_hbm, slope_hbm, forward_hbm, backward_hbm,
    out_ref,
    green_buf, column_buf, slope_buf, forward_buf, backward_buf, spectrum_re, spectrum_im,
    sums, charged, weight_rows, grid_spec, momenta_all, forward_src, forward_dst, kick_src, kick_dst, last_src, last_dst,
    load_sem, send_mom, recv_mom, send_fwd, recv_fwd, send_kick, recv_kick, send_last, recv_last,
):
    columns, planes, extent, particles = sizes
    period = 2 * extent
    quarter = period // 4
    count = extent // GROUP
    tiles = particles // LANES
    width = particles // planes
    bf16 = jnp.bfloat16

    c = lax.axis_index("cuts")
    t = lax.axis_index("tr")
    rank = lax.rem(t, GROUP)
    base = t - rank
    ahead = lax.rem(c + columns - 2, columns)
    behind = lax.rem(c + 2, columns)
    home = lax.rem(c + 2 * (SECTIONS - 1), columns)
    origin = lax.rem(c + columns - 2 * (SECTIONS - 1), columns)

    def member(step):
        return base + lax.rem(rank + step, GROUP)

    green_at = [pltpu.make_async_copy(green_ref.at[:, pl.ds(h * extent, extent)], green_buf.at[h], load_sem.at[h]) for h in range(2)]
    column_at = pltpu.make_async_copy(column_hbm.at[rank], column_buf, load_sem.at[2])
    slope_at = pltpu.make_async_copy(slope_hbm.at[rank], slope_buf, load_sem.at[3])
    forward_at = pltpu.make_async_copy(forward_hbm, forward_buf, load_sem.at[4])
    backward_at = pltpu.make_async_copy(backward_hbm, backward_buf, load_sem.at[5])
    for load in (column_at, green_at[0], green_at[1], forward_at, backward_at, slope_at):
        load.start()

    barrier = pltpu.get_barrier_semaphore()

    def greet(column, plane):
        pl.semaphore_signal(barrier, inc=1, device_id={"cuts": column, "tr": plane}, device_id_type=MESH)

    for step in range(1, planes):
        greet(c, lax.rem(t + step, planes))
    for step in range(planes):
        greet(ahead, lax.rem(t + step, planes))
        greet(behind, lax.rem(t + step, planes))
    for step in range(GROUP):
        greet(home, member(step))
        greet(origin, member(step))
    greeted = planes - 1 + 2 * planes + 2 * GROUP

    def packed(ref, lead):
        return jnp.concatenate([ref[lead + (slice(LANES * i, LANES * (i + 1)),)][None] for i in range(tiles)], axis=0)

    position = [
        [packed(cells_ref, (b, 0, d)).astype(jnp.float32) + packed(offsets_ref, (b, 0, d)) for d in range(2)] for b in range(2)
    ]
    charge = [packed(charges_ref, (b, 0)) for b in range(2)]
    momentum = [[None, None], [None, None]]

    def copy_to(source, target, send, receive, column, plane):
        return pltpu.make_async_remote_copy(
            src_ref=source, dst_ref=target, send_sem=send, recv_sem=receive,
            device_id={"cuts": column, "tr": plane}, device_id_type=MESH,
        )

    sends = []

    def forward_copy(section):
        return copy_to(forward_src.at[section], forward_dst.at[section], send_fwd.at[section], recv_fwd.at[section], ahead, t)

    def momenta_copy(b, step):
        column = c if b == 0 else ahead
        return copy_to(
            momenta_ref.at[b], momenta_all.at[b, step], send_mom.at[b, step], recv_mom.at[b, step], column, lax.rem(t + step, planes)
        )

    def kick_copy(section, b, step):
        column = c if b == 0 else ahead
        return copy_to(
            kick_src.at[section, b], kick_dst.at[section, b, step], send_kick.at[section, b, step], recv_kick.at[section, b, step],
            column, member(step),
        )

    def last_copy(b, step):
        column = c if b == 0 else home
        plane = member(step)
        return copy_to(
            last_src.at[b, (plane * width) // LANES], last_dst.at[b, step], send_last.at[b, step], recv_last.at[b, step], column, plane
        )

    def put_forward(section, parts):
        for i, part in enumerate(parts):
            forward_src[section, i] = part

    def hats(place, tile):
        nodes = lax.broadcasted_iota(jnp.int32, (extent, LANES), 0).astype(jnp.float32)
        distance = jnp.abs(nodes - place[tile : tile + 1, :])
        return jnp.maximum(1.0 - distance, 0.0).astype(bf16)

    def hat_pair(place, pair):
        return jnp.concatenate([hats(place, 2 * pair), hats(place, 2 * pair + 1)], axis=1)

    def column_sums(b):
        for pair in range(tiles // 2):
            span = slice(2 * LANES * pair, 2 * LANES * (pair + 1))
            found = dot(column_buf[...], hat_pair(position[b][1], pair))
            sums[b, :, span] = found
            heavy = jnp.concatenate([charge[b][2 * pair : 2 * pair + 1], charge[b][2 * pair + 1 : 2 * pair + 2]], axis=1)
            charged[b, :, span] = (found * heavy).astype(bf16)
            weight_rows[b, :, span] = hat_pair(position[b][0], pair)

    def column_spectrum(b):
        grid_spec[...] = dot_t(charged[b], weight_rows[b])

    def quarter_turns(re, im):
        if len(re) == 2:
            return [
                (re[0] + re[1], im[0] + im[1]),
                (re[0] + im[1], im[0] - re[1]),
                (re[0] - re[1], im[0] - im[1]),
                (re[0] - im[1], im[0] + re[1]),
            ]
        even_re, odd_re = re[0] + re[2], re[1] + re[3]
        even_im, odd_im = im[0] + im[2], im[1] + im[3]
        far_re, turn_re = re[0] - re[2], re[1] - re[3]
        far_im, turn_im = im[0] - im[2], im[1] - im[3]
        return [
            (even_re + odd_re, even_im + odd_im),
            (far_re + turn_im, far_im - turn_re),
            (even_re - odd_re, even_im - odd_im),
            (far_re - turn_im, far_im + turn_re),
        ]

    def to_rows(pair, residue):
        both = dot(jnp.concatenate([pair[0], pair[1]], axis=0).astype(bf16), forward_buf[residue])
        real = both[:count, :quarter] + both[count:, quarter:]
        imag = both[count:, :quarter] - both[:count, quarter:]
        return real, imag

    def kernel_spectrum():
        for load in green_at:
            load.wait()
        near = dot_t(column_buf[...], green_buf[0].astype(bf16))
        far = dot_t(column_buf[...], green_buf[1].astype(bf16))
        sign = (1 - 2 * lax.rem(rank, 2)).astype(jnp.float32)
        re = near[:count] - sign * far[count:]
        im = near[count:] + sign * far[:count]
        quarters = [slice(quarter * m, quarter * (m + 1)) for m in range(4)]
        turns = quarter_turns([re[:, q] for q in quarters], [im[:, q] for q in quarters])
        scale = 2.0 / (period * period)
        for residue in range(4):
            real, imag = to_rows(turns[residue], residue)
            spectrum_re[residue] = real * scale
            spectrum_im[residue] = imag * scale

    def field_spectra():
        halves = [slice(0, quarter), slice(quarter, extent)]
        turns = quarter_turns([grid_spec[:count, h] for h in halves], [grid_spec[count:, h] for h in halves])
        back = []
        for residue in range(4):
            x_re, x_im = to_rows(turns[residue], residue)
            k_re, k_im = spectrum_re[residue], spectrum_im[residue]
            z = jnp.concatenate([x_re * k_re - x_im * k_im, x_re * k_im + x_im * k_re], axis=0).astype(bf16)
            both = dot(z, backward_buf[residue])
            back.append((both[:count, :quarter] - both[count:, quarter:], both[count:, :quarter] + both[:count, quarter:]))
        (a_re, a_im), (b_re, b_im), (c_re, c_im), (d_re, d_im) = back
        even_re, even_im, odd_re, odd_im = a_re + c_re, a_im + c_im, b_re + d_re, b_im + d_im
        far_re, far_im, turn_re, turn_im = a_re - c_re, a_im - c_im, b_re - d_re, b_im - d_im
        v_re = jnp.concatenate([even_re + odd_re, far_re - turn_im], axis=1)
        v_im = jnp.concatenate([even_im + odd_im, far_im + turn_re], axis=1)
        v = jnp.concatenate([v_re, v_im], axis=0)
        along_rows = 0.5 * (pltpu.roll(v, 1, 1) - pltpu.roll(v, extent - 1, 1))
        slope = jnp.concatenate([slope_buf[...]] * (extent // LANES), axis=1)
        return jnp.concatenate([along_rows.astype(bf16), (slope * v_im).astype(bf16), (-slope * v_re).astype(bf16)], axis=0)

    def kicks_on(b, spectra):
        rows = [[], []]
        for pair in range(tiles // 2):
            span = slice(2 * LANES * pair, 2 * LANES * (pair + 1))
            reached = dot(spectra, weight_rows[b, :, span])
            own = sums[b, :, span]
            for d in range(2):
                terms = reached[2 * count * d : 2 * count * (d + 1)] * own
                total = jnp.sum(jnp.sum(terms.reshape(2 * count // 8, 8, 2 * LANES), axis=0), axis=0, keepdims=True)
                rows[d] += [total[:, :LANES], total[:, LANES:]]
        return [jnp.concatenate(rows[d], axis=0) for d in range(2)]

    def send_kicks(section, b, parts):
        own = jnp.concatenate(parts, axis=0).astype(bf16)
        kick_src[section, b] = own
        for step in range(1 if b == 0 else 0, GROUP):
            copy = kick_copy(section, b, step)
            copy.start()
            sends.append(copy)
        return own

    def whole_momenta(b):
        for step in range(1 if b == 0 else 0, planes):
            momenta_copy(b, step).wait_recv()
        if b == 0:
            momenta_all[0, 0] = momenta_ref[0]
        result = []
        for d in range(2):
            each = []
            for plane in range(planes):
                slot = lax.rem(t - plane + planes, planes)
                each.append(momenta_all[b, slot, 0, d][None])
            share = LANES // width
            rows = [each[i] if share == 1 else jnp.concatenate(each[share * i : share * (i + 1)], axis=1) for i in range(tiles)]
            result.append(jnp.concatenate(rows, axis=0))
        return result

    def arrive(section, b, own):
        if b == 0:
            if section == 0:
                momentum[0] = whole_momenta(0)
            old = [position[0][d] + DRIFT * momentum[0][d] for d in range(2)]
        else:
            forward_copy(section).wait_recv()
            old = [forward_dst[section, d] for d in range(2)]
            momentum[1] = whole_momenta(1) if section == 0 else [forward_dst[section, 2 + d] for d in range(2)]
            charge[1] = forward_dst[section, 4]
            if section == 0:
                old = [old[d] + DRIFT * momentum[1][d] for d in range(2)]
        total = own.astype(jnp.float32) if b == 0 else None
        for step in range(1 if b == 0 else 0, GROUP):
            kick_copy(section, b, step).wait_recv()
            part = kick_dst[section, b, step].astype(jnp.float32)
            total = part if total is None else total + part
        for d in range(2):
            kick = total[tiles * d : tiles * (d + 1)]
            momentum[b][d] = momentum[b][d] + kick
            position[b][d] = jnp.clip(old[d] + DRIFT * kick, 1.0, extent - 2.0 - 1.0 / 64.0)
        if b == 1 and section + 1 < SECTIONS - 1:
            put_forward(section + 1, [position[1][d] + DRIFT * momentum[1][d] for d in range(2)] + momentum[1] + [charge[1]])
            copy = forward_copy(section + 1)
            copy.start()
            sends.append(copy)

    def send_last_kicks(b, parts):
        for i in range(tiles):
            rows = [parts[d][i : i + 1] for d in range(2)]
            last_src[b, i] = jnp.concatenate(rows + [jnp.zeros((6, LANES), jnp.float32)], axis=0)
        for step in range(1 if b == 0 else 0, GROUP):
            copy = last_copy(b, step)
            copy.start()
            sends.append(copy)

    def own_lanes(tile):
        share = LANES // width
        if share == 1:
            return tile
        place = lax.rem(t, share)
        result = tile[:, :width]
        for i in range(1, share):
            result = jnp.where(place == i, tile[:, width * i : width * (i + 1)], result)
        return result

    put_forward(0, position[1] + [jnp.zeros_like(charge[1])] * 2 + [charge[1]])
    column_at.wait()
    own_kicks = [None, None]
    first = 1
    for section in range(SECTIONS):
        second = 1 - first
        if section > 0:
            arrive(section - 1, first, own_kicks[first])
        column_sums(first)
        column_spectrum(first)
        if section == 0:
            for load in (forward_at, backward_at, slope_at):
                load.wait()
            kernel_spectrum()
        spectra = field_spectra()
        if section > 0:
            arrive(section - 1, second, own_kicks[second])
        column_sums(second)
        if section == 0:
            pl.semaphore_wait(barrier, greeted)
            copies = [forward_copy(0)] + [momenta_copy(b, step) for b in range(2) for step in range(1 - b, planes)]
            for copy in copies:
                copy.start()
            sends += copies
        for source, target in ((first, second), (second, first)):
            if source == second:
                column_spectrum(second)
                spectra = field_spectra()
            parts = kicks_on(target, spectra)
            if section + 1 < SECTIONS:
                own_kicks[target] = send_kicks(section, target, parts)
            else:
                share = 1.0 / GROUP
                send_last_kicks(target, [parts[d] + share * momentum[target][d] for d in range(2)])
        first = second

    for b in (1, 0):
        total = last_src[0, (t * width) // LANES] if b == 0 else None
        for step in range(1 if b == 0 else 0, GROUP):
            last_copy(b, step).wait_recv()
            total = last_dst[b, step] if total is None else total + last_dst[b, step]
        out_ref[b, 0] = own_lanes(total[0:2])
    for copy in sends:
        copy.wait_send()


def per_device(mesh_shape, cells, offsets, charges, momenta, green):
    columns, planes = mesh_shape
    period = green.shape[0]
    extent = period // 2
    quarter = period // 4
    particles = cells.shape[-1]
    tiles = particles // LANES
    count = extent // GROUP
    forward, backward = row_tables(period)
    column, slope = column_tables(period)
    vmem = pl.BlockSpec(memory_space=pltpu.VMEM)
    anywhere = pl.BlockSpec(memory_space=pl.ANY)
    dma = pltpu.SemaphoreType.DMA
    f32, bf16 = jnp.float32, jnp.bfloat16
    return pl.pallas_call(
        functools.partial(kernel, (columns, planes, extent, particles)),
        out_shape=jax.ShapeDtypeStruct(momenta.shape, momenta.dtype),
        in_specs=[vmem] * 4 + [anywhere] * 5,
        out_specs=vmem,
        scratch_shapes=[
            pltpu.VMEM((2, period, extent), f32),
            pltpu.VMEM((2 * count, extent), bf16),
            pltpu.VMEM((count, LANES), f32),
            pltpu.VMEM((4, quarter, 2 * quarter), bf16),
            pltpu.VMEM((4, quarter, 2 * quarter), bf16),
            pltpu.VMEM((4, count, quarter), f32),
            pltpu.VMEM((4, count, quarter), f32),
            pltpu.VMEM((2, 2 * count, particles), f32),
            pltpu.VMEM((2, 2 * count, particles), bf16),
            pltpu.VMEM((2, extent, particles), bf16),
            pltpu.VMEM((2 * count, extent), f32),
            pltpu.VMEM((2, planes, *momenta.shape[1:]), f32),
            pltpu.VMEM((SECTIONS - 1, 5, tiles, LANES), f32),
            pltpu.VMEM((SECTIONS - 1, 5, tiles, LANES), f32),
            pltpu.VMEM((SECTIONS - 1, 2, 2 * tiles, LANES), bf16),
            pltpu.VMEM((SECTIONS - 1, 2, GROUP, 2 * tiles, LANES), bf16),
            pltpu.VMEM((2, tiles, 8, LANES), f32),
            pltpu.VMEM((2, GROUP, 8, LANES), f32),
            dma((6,)),
            dma((2, planes)),
            dma((2, planes)),
            dma((SECTIONS - 1,)),
            dma((SECTIONS - 1,)),
            dma((SECTIONS - 1, 2, GROUP)),
            dma((SECTIONS - 1, 2, GROUP)),
            dma((2, GROUP)),
            dma((2, GROUP)),
        ],
        compiler_params=pltpu.CompilerParams(collective_id=0, has_side_effects=True, vmem_limit_bytes=60 * 1024 * 1024),
    )(cells, offsets, charges, momenta, green, column, slope, forward, backward)


def solution(mesh):
    return jax.shard_map(
        functools.partial(per_device, (mesh.shape["cuts"], mesh.shape["tr"])),
        mesh=mesh,
        in_specs=(
            P(None, "cuts", None, None),
            P(None, "cuts", None, None),
            P(None, "cuts", None),
            P(None, "cuts", None, "tr"),
            P(),
        ),
        out_specs=P(None, "cuts", None, "tr"),
        check_vma=False,
    )
```

```python
import functools
import math

import jax
import jax.numpy as jnp
import numpy as np
from jax import lax
from jax.experimental import pallas as pl
from jax.experimental.pallas import tpu as pltpu
from jax.sharding import PartitionSpec as P

SECTIONS = 4
GROUP = 4
LANES = 128
DRIFT = 0.5
MESH = pl.DeviceIdType.MESH


def turns(angle_steps, period):
    angle = 2.0 * np.pi / period * (angle_steps % period)
    return np.stack([np.cos(angle), np.sin(angle)], axis=-3).astype(np.float32)


def row_tables(period):
    near = np.arange(period // 4)
    coarse, fine = np.arange(period // 32), np.arange(8)
    residue = np.arange(4)[:, None, None]
    frequency = 4 * near[None, None, :] + residue
    forward_coarse = turns(8 * coarse[None, :, None] * frequency, period)
    forward_fine = turns(fine[None, :, None] * frequency, period)
    backward_coarse = turns(32 * coarse[:, None] * near[None, :], period)
    backward_fine = turns((4 * fine[None, :, None] + residue) * near[None, None, :], period)
    return forward_coarse, forward_fine, backward_coarse, backward_fine


def column_tables(period):
    column = np.arange(period // 2)
    coarse = np.arange(period // 2 // GROUP // 8)
    fine = 2 * (GROUP * np.arange(8)[None, :] + np.arange(GROUP)[:, None]) + 1
    return turns(8 * GROUP * coarse[:, None] * column[None, :], period), turns(fine[:, :, None] * column, 2 * period)


def dot(left, right):
    return lax.dot_general(left, right, (((1,), (0,)), ((), ())), preferred_element_type=jnp.float32)


def dot_t(left, right):
    return lax.dot_general(left, right, (((1,), (1,)), ((), ())), preferred_element_type=jnp.float32)


def kernel(
    sizes,
    cells_ref, offsets_ref, charges_ref, momenta_ref, green_ref, column_hbm, column_fine_hbm, *row_hbm_and_rest,
):
    row_hbm = row_hbm_and_rest[:4]
    (

    out_ref, column_coarse, column_fine, *row_bufs_and_rest) = row_hbm_and_rest[4:]
    row_bufs = row_bufs_and_rest[:4]
    (green_buf, column_buf, slope_buf, forward_buf, backward_buf, spectrum_re, spectrum_im,
    sums, charged, weight_rows, grid_spec, momenta_all, forward_src, forward_dst, kick_src, kick_dst, last_src, last_dst,
    load_sem, send_mom, recv_mom, send_fwd, recv_fwd, send_kick, recv_kick, send_last, recv_last) = row_bufs_and_rest[4:]
    columns, planes, extent, particles = sizes
    period = 2 * extent
    quarter = period // 4
    count = extent // GROUP
    tiles = particles // LANES
    width = particles // planes
    bf16 = jnp.bfloat16

    c = lax.axis_index("cuts")
    t = lax.axis_index("tr")
    rank = lax.rem(t, GROUP)
    base = t - rank
    ahead = lax.rem(c + columns - 2, columns)
    behind = lax.rem(c + 2, columns)
    home = lax.rem(c + 2 * (SECTIONS - 1), columns)
    origin = lax.rem(c + columns - 2 * (SECTIONS - 1), columns)

    def member(step):
        return base + lax.rem(rank + step, GROUP)

    green_at = [pltpu.make_async_copy(green_ref.at[:, pl.ds(h * extent, extent)], green_buf.at[h], load_sem.at[h]) for h in range(2)]
    column_at = [
        pltpu.make_async_copy(column_hbm, column_coarse, load_sem.at[2]),
        pltpu.make_async_copy(column_fine_hbm.at[rank], column_fine, load_sem.at[3]),
    ]
    row_at = [pltpu.make_async_copy(row_hbm[i], row_bufs[i], load_sem.at[4 + i]) for i in range(4)]
    for load in column_at + green_at + row_at:
        load.start()

    barrier = pltpu.get_barrier_semaphore()

    def greet(column, plane):
        pl.semaphore_signal(barrier, inc=1, device_id={"cuts": column, "tr": plane}, device_id_type=MESH)

    for step in range(1, planes):
        greet(c, lax.rem(t + step, planes))
    for step in range(GROUP):
        greet(ahead, member(step))
        greet(behind, member(step))
        greet(home, member(step))
        greet(origin, member(step))
    greeted = planes - 1 + 4 * GROUP

    def packed(ref, lead):
        return jnp.concatenate([ref[lead + (slice(LANES * i, LANES * (i + 1)),)][None] for i in range(tiles)], axis=0)

    position = [
        [packed(cells_ref, (b, 0, d)).astype(jnp.float32) + packed(offsets_ref, (b, 0, d)) for d in range(2)] for b in range(2)
    ]
    charge = [packed(charges_ref, (b, 0)) for b in range(2)]
    momentum = [[None, None], [None, None]]

    def copy_to(source, target, send, receive, column, plane):
        return pltpu.make_async_remote_copy(
            src_ref=source, dst_ref=target, send_sem=send, recv_sem=receive,
            device_id={"cuts": column, "tr": plane}, device_id_type=MESH,
        )

    sends = []

    def forward_copy(section):
        return copy_to(forward_src.at[section], forward_dst.at[section], send_fwd.at[section], recv_fwd.at[section], ahead, t)

    def momenta_copy(step):
        return copy_to(momenta_ref, momenta_all.at[step], send_mom.at[step], recv_mom.at[step], c, lax.rem(t + step, planes))

    def kick_copy(section, b, step):
        column = c if b == 0 else ahead
        return copy_to(
            kick_src.at[section, b], kick_dst.at[section, b, step], send_kick.at[section, b, step], recv_kick.at[section, b, step],
            column, member(step),
        )

    def last_copy(b, step):
        column = c if b == 0 else home
        plane = member(step)
        return copy_to(
            last_src.at[b, (plane * width) // LANES], last_dst.at[b, step], send_last.at[b, step], recv_last.at[b, step], column, plane
        )

    def turned(coarse_ref, fine_ref, lead, first):
        far_cos, far_sin = coarse_ref[lead[0] + (0, slice(first, first + 1))], coarse_ref[lead[0] + (1, slice(first, first + 1))]
        near_cos, near_sin = fine_ref[lead[1] + (0,)], fine_ref[lead[1] + (1,)]
        return far_cos * near_cos - far_sin * near_sin, far_sin * near_cos + far_cos * near_sin

    def fill_columns():
        for load in column_at:
            load.wait()
        cosines, sines = [], []
        for i in range(count // 8):
            cosine, sine = turned(column_coarse, column_fine, ((), ()), i)
            cosines.append(cosine.astype(bf16))
            sines.append((-sine).astype(bf16))
            slope_buf[8 * i : 8 * i + 8] = jnp.broadcast_to(sine[:, 1:2], (8, LANES))
        for i in range(0, count // 8, 2):
            column_buf[8 * i : 8 * i + 16] = jnp.concatenate(cosines[i : i + 2], axis=0)
            column_buf[count + 8 * i : count + 8 * i + 16] = jnp.concatenate(sines[i : i + 2], axis=0)

    def fill_rows():
        for load in row_at:
            load.wait()
        forward_coarse, forward_fine, backward_coarse, backward_fine = row_bufs
        for residue in range(4):
            for i in range(0, quarter // 8, 2):
                span = slice(8 * i, 8 * i + 16)
                for buf, coarse, fine, lead in (
                    (forward_buf, forward_coarse, forward_fine, ((residue,), (residue,))),
                    (backward_buf, backward_coarse, backward_fine, ((), (residue,))),
                ):
                    one, two = turned(coarse, fine, lead, i), turned(coarse, fine, lead, i + 1)
                    for part in range(2):
                        both = jnp.concatenate([one[part], two[part]], axis=0).astype(bf16)
                        buf[residue, span, quarter * part : quarter * (part + 1)] = both

    side = 16
    nodes = lax.broadcasted_iota(jnp.int32, (side, LANES), 0).astype(jnp.float32)

    def hats(place, tile):
        place = place[tile : tile + 1, :]
        cell = jnp.floor(place)
        high = place - cell
        block = jnp.floor(cell * (1.0 / side))
        node = cell - side * block
        here = jnp.where(nodes == node, 1.0 - high, jnp.where(nodes == node + 1.0, high, 0.0)).astype(bf16)
        following = jnp.where(nodes == node - (side - 1.0), high, 0.0).astype(bf16)
        number = jnp.broadcast_to(block, (side, LANES)).astype(bf16)
        none = jnp.zeros((side, LANES), bf16)
        before, blocks = None, []
        for k in range(extent // side):
            mine = number == jnp.asarray(k, bf16)
            rest = none if before is None else jnp.where(before, following, none)
            blocks.append(jnp.where(mine, here, rest))
            before = mine
        return jnp.concatenate(blocks, axis=0)

    def hat_pair(place, pair):
        return jnp.concatenate([hats(place, 2 * pair), hats(place, 2 * pair + 1)], axis=1)

    def column_sums(b):
        for pair in range(tiles // 2):
            span = slice(2 * LANES * pair, 2 * LANES * (pair + 1))
            found = dot(column_buf[...], hat_pair(position[b][1], pair))
            sums[b, :, span] = found
            heavy = jnp.concatenate([charge[b][2 * pair : 2 * pair + 1], charge[b][2 * pair + 1 : 2 * pair + 2]], axis=1)
            charged[b, :, span] = (found * heavy).astype(bf16)
            weight_rows[b, :, span] = hat_pair(position[b][0], pair)

    def column_spectrum(b):
        grid_spec[...] = dot_t(charged[b], weight_rows[b])

    def quarter_turns(re, im):
        if len(re) == 2:
            return [
                (re[0] + re[1], im[0] + im[1]),
                (re[0] + im[1], im[0] - re[1]),
                (re[0] - re[1], im[0] - im[1]),
                (re[0] - im[1], im[0] + re[1]),
            ]
        even_re, odd_re = re[0] + re[2], re[1] + re[3]
        even_im, odd_im = im[0] + im[2], im[1] + im[3]
        far_re, turn_re = re[0] - re[2], re[1] - re[3]
        far_im, turn_im = im[0] - im[2], im[1] - im[3]
        return [
            (even_re + odd_re, even_im + odd_im),
            (far_re + turn_im, far_im - turn_re),
            (even_re - odd_re, even_im - odd_im),
            (far_re - turn_im, far_im + turn_re),
        ]

    def to_rows(pair, residue):
        both = dot(jnp.concatenate([pair[0], pair[1]], axis=0).astype(bf16), forward_buf[residue])
        real = both[:count, :quarter] + both[count:, quarter:]
        imag = both[count:, :quarter] - both[:count, quarter:]
        return real, imag

    def kernel_spectrum():
        for load in green_at:
            load.wait()
        near = dot_t(column_buf[...], green_buf[0].astype(bf16))
        far = dot_t(column_buf[...], green_buf[1].astype(bf16))
        sign = (1 - 2 * lax.rem(rank, 2)).astype(jnp.float32)
        re = near[:count] - sign * far[count:]
        im = near[count:] + sign * far[:count]
        quarters = [slice(quarter * m, quarter * (m + 1)) for m in range(4)]
        turns = quarter_turns([re[:, q] for q in quarters], [im[:, q] for q in quarters])
        scale = 2.0 / (period * period)
        for residue in range(4):
            real, imag = to_rows(turns[residue], residue)
            spectrum_re[residue] = real * scale
            spectrum_im[residue] = imag * scale

    def field_spectra():
        halves = [slice(0, quarter), slice(quarter, extent)]
        turns = quarter_turns([grid_spec[:count, h] for h in halves], [grid_spec[count:, h] for h in halves])
        back = []
        for residue in range(4):
            x_re, x_im = to_rows(turns[residue], residue)
            k_re, k_im = spectrum_re[residue], spectrum_im[residue]
            z = jnp.concatenate([x_re * k_re - x_im * k_im, x_re * k_im + x_im * k_re], axis=0).astype(bf16)
            both = dot(z, backward_buf[residue])
            back.append((both[:count, :quarter] - both[count:, quarter:], both[count:, :quarter] + both[:count, quarter:]))
        (a_re, a_im), (b_re, b_im), (c_re, c_im), (d_re, d_im) = back
        even_re, even_im, odd_re, odd_im = a_re + c_re, a_im + c_im, b_re + d_re, b_im + d_im
        far_re, far_im, turn_re, turn_im = a_re - c_re, a_im - c_im, b_re - d_re, b_im - d_im
        v_re = jnp.concatenate([even_re + odd_re, far_re - turn_im], axis=1)
        v_im = jnp.concatenate([even_im + odd_im, far_im + turn_re], axis=1)
        v = jnp.concatenate([v_re, v_im], axis=0)
        along_rows = 0.5 * (pltpu.roll(v, 1, 1) - pltpu.roll(v, extent - 1, 1))
        slope = jnp.concatenate([slope_buf[...]] * (extent // LANES), axis=1)
        return jnp.concatenate([along_rows.astype(bf16), (slope * v_im).astype(bf16), (-slope * v_re).astype(bf16)], axis=0)

    def kicks_on(b, spectra):
        rows = [[], []]
        for pair in range(tiles // 2):
            span = slice(2 * LANES * pair, 2 * LANES * (pair + 1))
            reached = dot(spectra, weight_rows[b, :, span])
            own = sums[b, :, span]
            for d in range(2):
                terms = reached[2 * count * d : 2 * count * (d + 1)] * own
                total = jnp.sum(jnp.sum(terms.reshape(2 * count // 8, 8, 2 * LANES), axis=0), axis=0, keepdims=True)
                rows[d] += [total[:, :LANES], total[:, LANES:]]
        return [jnp.concatenate(rows[d], axis=0) for d in range(2)]

    def send_kicks(section, b, parts):
        own = jnp.concatenate(parts, axis=0).astype(bf16)
        kick_src[section, b] = own
        for step in range(1 if b == 0 else 0, GROUP):
            copy = kick_copy(section, b, step)
            copy.start()
            sends.append(copy)
        return own

    def whole_momenta():
        momenta_all[0] = momenta_ref[...]
        for step in range(1, planes):
            momenta_copy(step).wait_recv()
        share = LANES // width
        for b in range(2):
            for d in range(2):
                each = [momenta_all[lax.rem(t - plane + planes, planes), b, 0, d][None] for plane in range(planes)]
                rows = [jnp.concatenate(each[share * i : share * (i + 1)], axis=1) for i in range(tiles)]
                momentum[b][d] = jnp.concatenate(rows, axis=0)

    def pass_on(section):
        parts = [position[1][d] + DRIFT * momentum[1][d] for d in range(2)] + momentum[1] + [charge[1]]
        for i, part in enumerate(parts):
            forward_src[section, i] = part
        copy = forward_copy(section)
        copy.start()
        sends.append(copy)

    def arrive(section, b, own):
        if section == 0 and b == 0:
            whole_momenta()
            pass_on(0)
        if b == 0:
            old = [position[0][d] + DRIFT * momentum[0][d] for d in range(2)]
        else:
            forward_copy(section).wait_recv()
            old = [forward_dst[section, d] for d in range(2)]
            momentum[1] = [forward_dst[section, 2 + d] for d in range(2)]
            charge[1] = forward_dst[section, 4]
        total = own.astype(jnp.float32) if b == 0 else None
        for step in range(1 if b == 0 else 0, GROUP):
            kick_copy(section, b, step).wait_recv()
            part = kick_dst[section, b, step].astype(jnp.float32)
            total = part if total is None else total + part
        for d in range(2):
            kick = total[tiles * d : tiles * (d + 1)]
            momentum[b][d] = momentum[b][d] + kick
            position[b][d] = jnp.clip(old[d] + DRIFT * kick, 1.0, extent - 2.0 - 1.0 / 64.0)
        if b == 1 and section + 1 < SECTIONS - 1:
            pass_on(section + 1)

    def send_last_kicks(b, parts):
        for i in range(tiles):
            rows = [parts[d][i : i + 1] for d in range(2)]
            last_src[b, i] = jnp.concatenate(rows + [jnp.zeros((6, LANES), jnp.float32)], axis=0)
        for step in range(1 if b == 0 else 0, GROUP):
            copy = last_copy(b, step)
            copy.start()
            sends.append(copy)

    def own_lanes(tile):
        share = LANES // width
        if share == 1:
            return tile
        place = lax.rem(t, share)
        result = tile[:, :width]
        for i in range(1, share):
            result = jnp.where(place == i, tile[:, width * i : width * (i + 1)], result)
        return result

    fill_columns()
    own_kicks = [None, None]
    first = 1
    for section in range(SECTIONS):
        second = 1 - first
        if section > 0:
            arrive(section - 1, first, own_kicks[first])
        column_sums(first)
        column_spectrum(first)
        if section == 0:
            fill_rows()
            kernel_spectrum()
        spectra = field_spectra()
        if section > 0:
            arrive(section - 1, second, own_kicks[second])
        column_sums(second)
        if section == 0:
            pl.semaphore_wait(barrier, greeted)
            copies = [momenta_copy(step) for step in range(1, planes)]
            for copy in copies:
                copy.start()
            sends += copies
        for source, target in ((first, second), (second, first)):
            if source == second:
                column_spectrum(second)
                spectra = field_spectra()
            parts = kicks_on(target, spectra)
            if section + 1 < SECTIONS:
                own_kicks[target] = send_kicks(section, target, parts)
            else:
                share = 1.0 / GROUP
                send_last_kicks(target, [parts[d] + share * momentum[target][d] for d in range(2)])
        first = second

    for b in (1, 0):
        total = last_src[0, (t * width) // LANES] if b == 0 else None
        for step in range(1 if b == 0 else 0, GROUP):
            last_copy(b, step).wait_recv()
            total = last_dst[b, step] if total is None else total + last_dst[b, step]
        out_ref[b, 0] = own_lanes(total[0:2])
    for copy in sends:
        copy.wait_send()


def per_device(mesh_shape, cells, offsets, charges, momenta, green):
    columns, planes = mesh_shape
    period = green.shape[0]
    extent = period // 2
    quarter = period // 4
    particles = cells.shape[-1]
    tiles = particles // LANES
    count = extent // GROUP
    tables = column_tables(period) + row_tables(period)
    vmem = pl.BlockSpec(memory_space=pltpu.VMEM)
    anywhere = pl.BlockSpec(memory_space=pl.ANY)
    dma = pltpu.SemaphoreType.DMA
    f32, bf16 = jnp.float32, jnp.bfloat16
    return pl.pallas_call(
        functools.partial(kernel, (columns, planes, extent, particles)),
        out_shape=jax.ShapeDtypeStruct(momenta.shape, momenta.dtype),
        in_specs=[vmem] * 4 + [anywhere] * 7,
        out_specs=vmem,
        scratch_shapes=[
            pltpu.VMEM(tables[0].shape, f32),
            pltpu.VMEM(tables[1].shape[1:], f32),
            *[pltpu.VMEM(table.shape, f32) for table in tables[2:]],
            pltpu.VMEM((2, period, extent), f32),
            pltpu.VMEM((2 * count, extent), bf16),
            pltpu.VMEM((count, LANES), f32),
            pltpu.VMEM((4, quarter, 2 * quarter), bf16),
            pltpu.VMEM((4, quarter, 2 * quarter), bf16),
            pltpu.VMEM((4, count, quarter), f32),
            pltpu.VMEM((4, count, quarter), f32),
            pltpu.VMEM((2, 2 * count, particles), f32),
            pltpu.VMEM((2, 2 * count, particles), bf16),
            pltpu.VMEM((2, extent, particles), bf16),
            pltpu.VMEM((2 * count, extent), f32),
            pltpu.VMEM((planes, *momenta.shape), f32),
            pltpu.VMEM((SECTIONS - 1, 5, tiles, LANES), f32),
            pltpu.VMEM((SECTIONS - 1, 5, tiles, LANES), f32),
            pltpu.VMEM((SECTIONS - 1, 2, 2 * tiles, LANES), bf16),
            pltpu.VMEM((SECTIONS - 1, 2, GROUP, 2 * tiles, LANES), bf16),
            pltpu.VMEM((2, tiles, 8, LANES), f32),
            pltpu.VMEM((2, GROUP, 8, LANES), f32),
            dma((8,)),
            dma((planes,)),
            dma((planes,)),
            dma((SECTIONS - 1,)),
            dma((SECTIONS - 1,)),
            dma((SECTIONS - 1, 2, GROUP)),
            dma((SECTIONS - 1, 2, GROUP)),
            dma((2, GROUP)),
            dma((2, GROUP)),
        ],
        compiler_params=pltpu.CompilerParams(collective_id=0, has_side_effects=True, vmem_limit_bytes=60 * 1024 * 1024),
    )(cells, offsets, charges, momenta, green, *tables)


def solution(mesh):
    return jax.shard_map(
        functools.partial(per_device, (mesh.shape["cuts"], mesh.shape["tr"])),
        mesh=mesh,
        in_specs=(
            P(None, "cuts", None, None),
            P(None, "cuts", None, None),
            P(None, "cuts", None),
            P(None, "cuts", None, "tr"),
            P(),
        ),
        out_specs=P(None, "cuts", None, "tr"),
        check_vma=False,
    )
```

```python
import functools
import math

import jax
import jax.numpy as jnp
import numpy as np
from jax import lax
from jax.experimental import pallas as pl
from jax.experimental.pallas import tpu as pltpu
from jax.sharding import PartitionSpec as P

SECTIONS = 4
GROUP = 4
LANES = 128
DRIFT = 0.5
MESH = pl.DeviceIdType.MESH


def turns(angle_steps, period):
    angle = 2.0 * np.pi / period * (angle_steps % period)
    return np.stack([np.cos(angle), np.sin(angle)], axis=-3).astype(np.float32)


def row_tables(period):
    near = np.arange(period // 4)
    coarse, fine = np.arange(period // 32), np.arange(8)
    residue = np.arange(4)[:, None, None]
    frequency = 4 * near[None, None, :] + residue
    forward_coarse = turns(8 * coarse[None, :, None] * frequency, period)
    forward_fine = turns(fine[None, :, None] * frequency, period)
    backward_coarse = turns(32 * coarse[:, None] * near[None, :], period)
    backward_fine = turns((4 * fine[None, :, None] + residue) * near[None, None, :], period)
    return forward_coarse, forward_fine, backward_coarse, backward_fine


def column_tables(period):
    column = np.arange(period // 2)
    coarse = np.arange(period // 2 // GROUP // 8)
    fine = 2 * (GROUP * np.arange(8)[None, :] + np.arange(GROUP)[:, None]) + 1
    return turns(8 * GROUP * coarse[:, None] * column[None, :], period), turns(fine[:, :, None] * column, 2 * period)


def dot(left, right):
    return lax.dot_general(left, right, (((1,), (0,)), ((), ())), preferred_element_type=jnp.float32)


def dot_t(left, right):
    return lax.dot_general(left, right, (((1,), (1,)), ((), ())), preferred_element_type=jnp.float32)


def kernel(
    sizes,
    cells_ref, offsets_ref, charges_ref, momenta_ref, green_ref, column_hbm, column_fine_hbm, *row_hbm_and_rest,
):
    row_hbm = row_hbm_and_rest[:4]
    (

    out_ref, column_coarse, column_fine, *row_bufs_and_rest) = row_hbm_and_rest[4:]
    row_bufs = row_bufs_and_rest[:4]
    (green_buf, column_buf, slope_buf, forward_buf, backward_buf, spectrum_re, spectrum_im,
    sums, charged, weight_rows, grid_spec, momenta_all, forward_src, forward_dst, kick_src, kick_dst, last_src, last_dst,
    load_sem, send_mom, recv_mom, send_relay, recv_relay, send_fwd, recv_fwd, send_kick, recv_kick, send_last, recv_last) = row_bufs_and_rest[4:]
    columns, planes, extent, particles = sizes
    period = 2 * extent
    quarter = period // 4
    count = extent // GROUP
    tiles = particles // LANES
    width = particles // planes
    bf16 = jnp.bfloat16

    c = lax.axis_index("cuts")
    t = lax.axis_index("tr")
    rank = lax.rem(t, GROUP)
    base = t - rank
    ahead = lax.rem(c + columns - 2, columns)
    behind = lax.rem(c + 2, columns)
    home = lax.rem(c + 2 * (SECTIONS - 1), columns)
    origin = lax.rem(c + columns - 2 * (SECTIONS - 1), columns)

    def member(step):
        return base + lax.rem(rank + step, GROUP)

    green_at = [pltpu.make_async_copy(green_ref.at[:, pl.ds(h * extent, extent)], green_buf.at[h], load_sem.at[h]) for h in range(2)]
    column_at = [
        pltpu.make_async_copy(column_hbm, column_coarse, load_sem.at[2]),
        pltpu.make_async_copy(column_fine_hbm.at[rank], column_fine, load_sem.at[3]),
    ]
    row_at = [pltpu.make_async_copy(row_hbm[i], row_bufs[i], load_sem.at[4 + i]) for i in range(4)]
    for load in column_at + green_at + row_at:
        load.start()

    barrier = pltpu.get_barrier_semaphore()

    def greet(column, plane):
        pl.semaphore_signal(barrier, inc=1, device_id={"cuts": column, "tr": plane}, device_id_type=MESH)

    half = planes // 4
    reach = max(half, GROUP - 1)
    for step in range(-reach, reach + 1):
        plane = lax.rem(t + step + planes, planes)
        if step != 0:
            greet(c, plane)
        greet(ahead, plane)
        greet(behind, plane)
    for step in range(GROUP):
        greet(home, member(step))
        greet(origin, member(step))
    greeted = 3 * (2 * reach + 1) - 1 + 2 * GROUP

    def packed(ref, lead):
        return jnp.concatenate([ref[lead + (slice(LANES * i, LANES * (i + 1)),)][None] for i in range(tiles)], axis=0)

    position = [
        [packed(cells_ref, (b, 0, d)).astype(jnp.float32) + packed(offsets_ref, (b, 0, d)) for d in range(2)] for b in range(2)
    ]
    charge = [packed(charges_ref, (b, 0)) for b in range(2)]
    momentum = [[None, None], [None, None]]

    def copy_to(source, target, send, receive, column, plane):
        return pltpu.make_async_remote_copy(
            src_ref=source, dst_ref=target, send_sem=send, recv_sem=receive,
            device_id={"cuts": column, "tr": plane}, device_id_type=MESH,
        )

    sends = []

    def forward_copy(section):
        return copy_to(forward_src.at[section], forward_dst.at[section], send_fwd.at[section], recv_fwd.at[section], ahead, t)

    def momenta_copy(b, step):
        slot = 2 * half - step
        return copy_to(
            momenta_ref.at[b], momenta_all.at[b, slot], send_mom.at[b, slot], recv_mom.at[b, slot],
            c if b == 0 else ahead, lax.rem(t + step + planes, planes),
        )

    near_steps = [[step for step in range(-half, half + 1) if b == 1 or step != 0] for b in range(2)]

    def relay_copy(b, up):
        first, last, target = (half, 2 * half, 0) if up else (2 * half + 1, 3 * half, 3 * half + 1)
        return copy_to(
            momenta_all.at[b, first:last], momenta_all.at[b, target : target + last - first],
            send_relay.at[b, int(up)], recv_relay.at[b, int(up)],
            c, lax.rem(t + (half if up else planes - half), planes),
        )

    def kick_copy(section, b, step):
        column = c if b == 0 else ahead
        return copy_to(
            kick_src.at[section, b], kick_dst.at[section, b, step], send_kick.at[section, b, step], recv_kick.at[section, b, step],
            column, member(step),
        )

    def last_copy(b, step):
        column = c if b == 0 else home
        plane = member(step)
        return copy_to(
            last_src.at[b, (plane * width) // LANES], last_dst.at[b, step], send_last.at[b, step], recv_last.at[b, step], column, plane
        )

    def turned(coarse_ref, fine_ref, lead, first):
        far_cos, far_sin = coarse_ref[lead[0] + (0, slice(first, first + 1))], coarse_ref[lead[0] + (1, slice(first, first + 1))]
        near_cos, near_sin = fine_ref[lead[1] + (0,)], fine_ref[lead[1] + (1,)]
        return far_cos * near_cos - far_sin * near_sin, far_sin * near_cos + far_cos * near_sin

    def fill_columns():
        for load in column_at:
            load.wait()
        cosines, sines = [], []
        for i in range(count // 8):
            cosine, sine = turned(column_coarse, column_fine, ((), ()), i)
            cosines.append(cosine.astype(bf16))
            sines.append((-sine).astype(bf16))
            slope_buf[8 * i : 8 * i + 8] = jnp.broadcast_to(sine[:, 1:2], (8, LANES))
        for i in range(0, count // 8, 2):
            column_buf[8 * i : 8 * i + 16] = jnp.concatenate(cosines[i : i + 2], axis=0)
            column_buf[count + 8 * i : count + 8 * i + 16] = jnp.concatenate(sines[i : i + 2], axis=0)

    def fill_rows():
        for load in row_at:
            load.wait()
        forward_coarse, forward_fine, backward_coarse, backward_fine = row_bufs
        for residue in range(4):
            for i in range(0, quarter // 8, 2):
                span = slice(8 * i, 8 * i + 16)
                for buf, coarse, fine, lead in (
                    (forward_buf, forward_coarse, forward_fine, ((residue,), (residue,))),
                    (backward_buf, backward_coarse, backward_fine, ((), (residue,))),
                ):
                    one, two = turned(coarse, fine, lead, i), turned(coarse, fine, lead, i + 1)
                    for part in range(2):
                        both = jnp.concatenate([one[part], two[part]], axis=0).astype(bf16)
                        buf[residue, span, quarter * part : quarter * (part + 1)] = both

    side = 16
    nodes = lax.broadcasted_iota(jnp.int32, (side, LANES), 0).astype(jnp.float32)

    def hats(place, tile):
        place = place[tile : tile + 1, :]
        cell = jnp.floor(place)
        high = place - cell
        block = jnp.floor(cell * (1.0 / side))
        node = cell - side * block
        here = jnp.where(nodes == node, 1.0 - high, jnp.where(nodes == node + 1.0, high, 0.0)).astype(bf16)
        following = jnp.where(nodes == node - (side - 1.0), high, 0.0).astype(bf16)
        number = jnp.broadcast_to(block, (side, LANES)).astype(bf16)
        none = jnp.zeros((side, LANES), bf16)
        before, blocks = None, []
        for k in range(extent // side):
            mine = number == jnp.asarray(k, bf16)
            rest = none if before is None else jnp.where(before, following, none)
            blocks.append(jnp.where(mine, here, rest))
            before = mine
        return jnp.concatenate(blocks, axis=0)

    def hat_pair(place, pair):
        return jnp.concatenate([hats(place, 2 * pair), hats(place, 2 * pair + 1)], axis=1)

    def column_sums(b):
        for pair in range(tiles // 2):
            span = slice(2 * LANES * pair, 2 * LANES * (pair + 1))
            found = dot(column_buf[...], hat_pair(position[b][1], pair))
            sums[b, :, span] = found
            heavy = jnp.concatenate([charge[b][2 * pair : 2 * pair + 1], charge[b][2 * pair + 1 : 2 * pair + 2]], axis=1)
            charged[b, :, span] = (found * heavy).astype(bf16)
            weight_rows[b, :, span] = hat_pair(position[b][0], pair)

    def column_spectrum(b):
        grid_spec[...] = dot_t(charged[b], weight_rows[b])

    def quarter_turns(re, im):
        if len(re) == 2:
            return [
                (re[0] + re[1], im[0] + im[1]),
                (re[0] + im[1], im[0] - re[1]),
                (re[0] - re[1], im[0] - im[1]),
                (re[0] - im[1], im[0] + re[1]),
            ]
        even_re, odd_re = re[0] + re[2], re[1] + re[3]
        even_im, odd_im = im[0] + im[2], im[1] + im[3]
        far_re, turn_re = re[0] - re[2], re[1] - re[3]
        far_im, turn_im = im[0] - im[2], im[1] - im[3]
        return [
            (even_re + odd_re, even_im + odd_im),
            (far_re + turn_im, far_im - turn_re),
            (even_re - odd_re, even_im - odd_im),
            (far_re - turn_im, far_im + turn_re),
        ]

    def to_rows(pair, residue):
        both = dot(jnp.concatenate([pair[0], pair[1]], axis=0).astype(bf16), forward_buf[residue])
        real = both[:count, :quarter] + both[count:, quarter:]
        imag = both[count:, :quarter] - both[:count, quarter:]
        return real, imag

    def kernel_spectrum():
        for load in green_at:
            load.wait()
        near = dot_t(column_buf[...], green_buf[0].astype(bf16))
        far = dot_t(column_buf[...], green_buf[1].astype(bf16))
        sign = (1 - 2 * lax.rem(rank, 2)).astype(jnp.float32)
        re = near[:count] - sign * far[count:]
        im = near[count:] + sign * far[:count]
        quarters = [slice(quarter * m, quarter * (m + 1)) for m in range(4)]
        turns = quarter_turns([re[:, q] for q in quarters], [im[:, q] for q in quarters])
        scale = 2.0 / (period * period)
        for residue in range(4):
            real, imag = to_rows(turns[residue], residue)
            spectrum_re[residue] = real * scale
            spectrum_im[residue] = imag * scale

    def field_spectra():
        halves = [slice(0, quarter), slice(quarter, extent)]
        turns = quarter_turns([grid_spec[:count, h] for h in halves], [grid_spec[count:, h] for h in halves])
        back = []
        for residue in range(4):
            x_re, x_im = to_rows(turns[residue], residue)
            k_re, k_im = spectrum_re[residue], spectrum_im[residue]
            z = jnp.concatenate([x_re * k_re - x_im * k_im, x_re * k_im + x_im * k_re], axis=0).astype(bf16)
            both = dot(z, backward_buf[residue])
            back.append((both[:count, :quarter] - both[count:, quarter:], both[count:, :quarter] + both[:count, quarter:]))
        (a_re, a_im), (b_re, b_im), (c_re, c_im), (d_re, d_im) = back
        even_re, even_im, odd_re, odd_im = a_re + c_re, a_im + c_im, b_re + d_re, b_im + d_im
        far_re, far_im, turn_re, turn_im = a_re - c_re, a_im - c_im, b_re - d_re, b_im - d_im
        v_re = jnp.concatenate([even_re + odd_re, far_re - turn_im], axis=1)
        v_im = jnp.concatenate([even_im + odd_im, far_im + turn_re], axis=1)
        v = jnp.concatenate([v_re, v_im], axis=0)
        along_rows = 0.5 * (pltpu.roll(v, 1, 1) - pltpu.roll(v, extent - 1, 1))
        slope = jnp.concatenate([slope_buf[...]] * (extent // LANES), axis=1)
        return jnp.concatenate([along_rows.astype(bf16), (slope * v_im).astype(bf16), (-slope * v_re).astype(bf16)], axis=0)

    def kicks_on(b, spectra):
        rows = [[], []]
        for pair in range(tiles // 2):
            span = slice(2 * LANES * pair, 2 * LANES * (pair + 1))
            reached = dot(spectra, weight_rows[b, :, span])
            own = sums[b, :, span]
            for d in range(2):
                terms = reached[2 * count * d : 2 * count * (d + 1)] * own
                total = jnp.sum(jnp.sum(terms.reshape(2 * count // 8, 8, 2 * LANES), axis=0), axis=0, keepdims=True)
                rows[d] += [total[:, :LANES], total[:, LANES:]]
        return [jnp.concatenate(rows[d], axis=0) for d in range(2)]

    def send_kicks(section, b, parts):
        own = jnp.concatenate(parts, axis=0).astype(bf16)
        kick_src[section, b] = own
        for step in range(1 if b == 0 else 0, GROUP):
            copy = kick_copy(section, b, step)
            copy.start()
            sends.append(copy)
        return own

    def relay_momenta():
        momenta_all[0, 2 * half] = momenta_ref[0]
        for b in range(2):
            for step in near_steps[b]:
                momenta_copy(b, step).wait_recv()
            for up in (True, False):
                copy = relay_copy(b, up)
                copy.start()
                sends.append(copy)

    def whole_momenta(b):
        for up in (True, False):
            relay_copy(b, up).wait_recv()
        share = LANES // width
        result = []
        for d in range(2):
            each = [momenta_all[b, lax.rem(plane - t + 2 * half + planes, planes), 0, d][None] for plane in range(planes)]
            rows = [jnp.concatenate(each[share * i : share * (i + 1)], axis=1) for i in range(tiles)]
            result.append(jnp.concatenate(rows, axis=0))
        return result

    def pass_on(section, parts):
        for i, part in enumerate(parts):
            forward_src[section, i] = part
        copy = forward_copy(section)
        copy.start()
        sends.append(copy)

    def arrive(section, b, own):
        if b == 0:
            if section == 0:
                momentum[0] = whole_momenta(0)
            old = [position[0][d] + DRIFT * momentum[0][d] for d in range(2)]
        else:
            forward_copy(section).wait_recv()
            old = [forward_dst[section, d] for d in range(2)]
            charge[1] = forward_dst[section, 4]
            if section == 0:
                momentum[1] = whole_momenta(1)
                old = [old[d] + DRIFT * momentum[1][d] for d in range(2)]
            else:
                momentum[1] = [forward_dst[section, 2 + d] for d in range(2)]
        total = own.astype(jnp.float32) if b == 0 else None
        for step in range(1 if b == 0 else 0, GROUP):
            kick_copy(section, b, step).wait_recv()
            part = kick_dst[section, b, step].astype(jnp.float32)
            total = part if total is None else total + part
        for d in range(2):
            kick = total[tiles * d : tiles * (d + 1)]
            momentum[b][d] = momentum[b][d] + kick
            position[b][d] = jnp.clip(old[d] + DRIFT * kick, 1.0, extent - 2.0 - 1.0 / 64.0)
        if b == 1 and section + 1 < SECTIONS - 1:
            pass_on(section + 1, [position[1][d] + DRIFT * momentum[1][d] for d in range(2)] + momentum[1] + [charge[1]])

    def send_last_kicks(b, parts):
        for i in range(tiles):
            rows = [parts[d][i : i + 1] for d in range(2)]
            last_src[b, i] = jnp.concatenate(rows + [jnp.zeros((6, LANES), jnp.float32)], axis=0)
        for step in range(1 if b == 0 else 0, GROUP):
            copy = last_copy(b, step)
            copy.start()
            sends.append(copy)

    def own_lanes(tile):
        share = LANES // width
        if share == 1:
            return tile
        place = lax.rem(t, share)
        result = tile[:, :width]
        for i in range(1, share):
            result = jnp.where(place == i, tile[:, width * i : width * (i + 1)], result)
        return result

    fill_columns()
    own_kicks = [None, None]
    first = 1
    for section in range(SECTIONS):
        second = 1 - first
        if section > 0:
            arrive(section - 1, first, own_kicks[first])
        column_sums(first)
        column_spectrum(first)
        if section == 0:
            fill_rows()
            kernel_spectrum()
        spectra = field_spectra()
        if section > 0:
            arrive(section - 1, second, own_kicks[second])
        column_sums(second)
        if section == 0:
            pl.semaphore_wait(barrier, greeted)
            pass_on(0, position[1] + [jnp.zeros_like(charge[1])] * 2 + [charge[1]])
            copies = [momenta_copy(b, step) for b in range(2) for step in near_steps[b]]
            for copy in copies:
                copy.start()
            sends += copies
        for source, target in ((first, second), (second, first)):
            if source == second:
                column_spectrum(second)
                spectra = field_spectra()
            parts = kicks_on(target, spectra)
            if section + 1 < SECTIONS:
                own_kicks[target] = send_kicks(section, target, parts)
            else:
                share = 1.0 / GROUP
                send_last_kicks(target, [parts[d] + share * momentum[target][d] for d in range(2)])
        if section == 0:
            relay_momenta()
        first = second

    for b in (1, 0):
        total = last_src[0, (t * width) // LANES] if b == 0 else None
        for step in range(1 if b == 0 else 0, GROUP):
            last_copy(b, step).wait_recv()
            total = last_dst[b, step] if total is None else total + last_dst[b, step]
        out_ref[b, 0] = own_lanes(total[0:2])
    for copy in sends:
        copy.wait_send()


def per_device(mesh_shape, cells, offsets, charges, momenta, green):
    columns, planes = mesh_shape
    period = green.shape[0]
    extent = period // 2
    quarter = period // 4
    particles = cells.shape[-1]
    tiles = particles // LANES
    count = extent // GROUP
    tables = column_tables(period) + row_tables(period)
    vmem = pl.BlockSpec(memory_space=pltpu.VMEM)
    anywhere = pl.BlockSpec(memory_space=pl.ANY)
    dma = pltpu.SemaphoreType.DMA
    f32, bf16 = jnp.float32, jnp.bfloat16
    return pl.pallas_call(
        functools.partial(kernel, (columns, planes, extent, particles)),
        out_shape=jax.ShapeDtypeStruct(momenta.shape, momenta.dtype),
        in_specs=[vmem] * 4 + [anywhere] * 7,
        out_specs=vmem,
        scratch_shapes=[
            pltpu.VMEM(tables[0].shape, f32),
            pltpu.VMEM(tables[1].shape[1:], f32),
            *[pltpu.VMEM(table.shape, f32) for table in tables[2:]],
            pltpu.VMEM((2, period, extent), f32),
            pltpu.VMEM((2 * count, extent), bf16),
            pltpu.VMEM((count, LANES), f32),
            pltpu.VMEM((4, quarter, 2 * quarter), bf16),
            pltpu.VMEM((4, quarter, 2 * quarter), bf16),
            pltpu.VMEM((4, count, quarter), f32),
            pltpu.VMEM((4, count, quarter), f32),
            pltpu.VMEM((2, 2 * count, particles), f32),
            pltpu.VMEM((2, 2 * count, particles), bf16),
            pltpu.VMEM((2, extent, particles), bf16),
            pltpu.VMEM((2 * count, extent), f32),
            pltpu.VMEM((2, planes, *momenta.shape[1:]), f32),
            pltpu.VMEM((SECTIONS - 1, 5, tiles, LANES), f32),
            pltpu.VMEM((SECTIONS - 1, 5, tiles, LANES), f32),
            pltpu.VMEM((SECTIONS - 1, 2, 2 * tiles, LANES), bf16),
            pltpu.VMEM((SECTIONS - 1, 2, GROUP, 2 * tiles, LANES), bf16),
            pltpu.VMEM((2, tiles, 8, LANES), f32),
            pltpu.VMEM((2, GROUP, 8, LANES), f32),
            dma((8,)),
            dma((2, planes)),
            dma((2, planes)),
            dma((2, 2)),
            dma((2, 2)),
            dma((SECTIONS - 1,)),
            dma((SECTIONS - 1,)),
            dma((SECTIONS - 1, 2, GROUP)),
            dma((SECTIONS - 1, 2, GROUP)),
            dma((2, GROUP)),
            dma((2, GROUP)),
        ],
        compiler_params=pltpu.CompilerParams(collective_id=0, has_side_effects=True, vmem_limit_bytes=60 * 1024 * 1024),
    )(cells, offsets, charges, momenta, green, *tables)


def solution(mesh):
    return jax.shard_map(
        functools.partial(per_device, (mesh.shape["cuts"], mesh.shape["tr"])),
        mesh=mesh,
        in_specs=(
            P(None, "cuts", None, None),
            P(None, "cuts", None, None),
            P(None, "cuts", None),
            P(None, "cuts", None, "tr"),
            P(),
        ),
        out_specs=P(None, "cuts", None, "tr"),
        check_vma=False,
    )
```

```python
import functools
import math

import jax
import jax.numpy as jnp
import numpy as np
from jax import lax
from jax.experimental import pallas as pl
from jax.experimental.pallas import tpu as pltpu
from jax.sharding import PartitionSpec as P

SECTIONS = 4
GROUP = 4
LANES = 128
DRIFT = 0.5
MESH = pl.DeviceIdType.MESH


def turns(angle_steps, period):
    angle = 2.0 * np.pi / period * (angle_steps % period)
    return np.stack([np.cos(angle), np.sin(angle)], axis=-3).astype(np.float32)


def row_tables(period):
    near = np.arange(period // 4)
    coarse, fine = np.arange(period // 32), np.arange(8)
    residue = np.arange(4)[:, None, None]
    frequency = 4 * near[None, None, :] + residue
    forward_coarse = turns(8 * coarse[None, :, None] * frequency, period)
    forward_fine = turns(fine[None, :, None] * frequency, period)
    backward_coarse = turns(32 * coarse[:, None] * near[None, :], period)
    backward_fine = turns((4 * fine[None, :, None] + residue) * near[None, None, :], period)
    return forward_coarse, forward_fine, backward_coarse, backward_fine


def column_tables(period):
    column = np.arange(period // 2)
    coarse = np.arange(period // 2 // GROUP // 8)
    fine = 2 * (GROUP * np.arange(8)[None, :] + np.arange(GROUP)[:, None]) + 1
    return turns(8 * GROUP * coarse[:, None] * column[None, :], period), turns(fine[:, :, None] * column, 2 * period)


def dot(left, right):
    return lax.dot_general(left, right, (((1,), (0,)), ((), ())), preferred_element_type=jnp.float32)


def dot_t(left, right):
    return lax.dot_general(left, right, (((1,), (1,)), ((), ())), preferred_element_type=jnp.float32)


def kernel(
    sizes,
    cells_ref, offsets_ref, charges_ref, momenta_ref, green_ref, column_hbm, column_fine_hbm, *row_hbm_and_rest,
):
    row_hbm = row_hbm_and_rest[:4]
    (

    out_ref, column_coarse, column_fine, *row_bufs_and_rest) = row_hbm_and_rest[4:]
    row_bufs = row_bufs_and_rest[:4]
    (green_buf, column_buf, slope_buf, forward_buf, backward_buf, spectrum_re, spectrum_im,
    sums, charged, weight_rows, grid_spec, turned_spec, product, scaled, returned, fields, near, far, momenta_all, forward_src, forward_dst, kick_src, kick_dst, last_src, last_dst,
    load_sem, send_mom, recv_mom, send_fwd, recv_fwd, send_kick, recv_kick, send_last, recv_last) = row_bufs_and_rest[4:]
    columns, planes, extent, particles = sizes
    period = 2 * extent
    quarter = period // 4
    count = extent // GROUP
    tiles = particles // LANES
    width = particles // planes
    bf16 = jnp.bfloat16

    c = lax.axis_index("cuts")
    t = lax.axis_index("tr")
    rank = lax.rem(t, GROUP)
    base = t - rank
    ahead = lax.rem(c + columns - 2, columns)
    behind = lax.rem(c + 2, columns)
    home = lax.rem(c + 2 * (SECTIONS - 1), columns)
    origin = lax.rem(c + columns - 2 * (SECTIONS - 1), columns)

    def member(step):
        return base + lax.rem(rank + step, GROUP)

    green_at = [pltpu.make_async_copy(green_ref.at[:, pl.ds(h * extent, extent)], green_buf.at[h], load_sem.at[h]) for h in range(2)]
    column_at = [
        pltpu.make_async_copy(column_hbm, column_coarse, load_sem.at[2]),
        pltpu.make_async_copy(column_fine_hbm.at[rank], column_fine, load_sem.at[3]),
    ]
    row_at = [pltpu.make_async_copy(row_hbm[i], row_bufs[i], load_sem.at[4 + i]) for i in range(4)]
    for load in column_at + green_at + row_at:
        load.start()

    barrier = pltpu.get_barrier_semaphore()

    def greet(column, plane):
        pl.semaphore_signal(barrier, inc=1, device_id={"cuts": column, "tr": plane}, device_id_type=MESH)

    for step in range(1, planes):
        greet(c, lax.rem(t + step, planes))
    for step in range(planes):
        greet(ahead, lax.rem(t + step, planes))
        greet(behind, lax.rem(t + step, planes))
    for step in range(GROUP):
        greet(home, member(step))
        greet(origin, member(step))
    greeted = planes - 1 + 2 * planes + 2 * GROUP

    def packed(ref, lead):
        return jnp.concatenate([ref[lead + (slice(LANES * i, LANES * (i + 1)),)][None] for i in range(tiles)], axis=0)

    position = [
        [packed(cells_ref, (b, 0, d)).astype(jnp.float32) + packed(offsets_ref, (b, 0, d)) for d in range(2)] for b in range(2)
    ]
    charge = [packed(charges_ref, (b, 0)) for b in range(2)]
    momentum = [[None, None], [None, None]]

    def copy_to(source, target, send, receive, column, plane):
        return pltpu.make_async_remote_copy(
            src_ref=source, dst_ref=target, send_sem=send, recv_sem=receive,
            device_id={"cuts": column, "tr": plane}, device_id_type=MESH,
        )

    sends = []

    def forward_copy(section):
        return copy_to(forward_src.at[section], forward_dst.at[section], send_fwd.at[section], recv_fwd.at[section], ahead, t)

    def momenta_copy(b, step):
        column = c if b == 0 else ahead
        return copy_to(
            momenta_ref.at[b], momenta_all.at[b, step], send_mom.at[b, step], recv_mom.at[b, step], column, lax.rem(t + step, planes)
        )

    def kick_copy(section, b, step):
        column = c if b == 0 else ahead
        return copy_to(
            kick_src.at[section, b], kick_dst.at[section, b, step], send_kick.at[section, b, step], recv_kick.at[section, b, step],
            column, member(step),
        )

    def last_copy(b, step):
        column = c if b == 0 else home
        plane = member(step)
        return copy_to(
            last_src.at[b, (plane * width) // LANES], last_dst.at[b, step], send_last.at[b, step], recv_last.at[b, step], column, plane
        )

    def turned(coarse_ref, fine_ref, lead, first):
        far_cos, far_sin = coarse_ref[lead[0] + (0, slice(first, first + 1))], coarse_ref[lead[0] + (1, slice(first, first + 1))]
        near_cos, near_sin = fine_ref[lead[1] + (0,)], fine_ref[lead[1] + (1,)]
        return far_cos * near_cos - far_sin * near_sin, far_sin * near_cos + far_cos * near_sin

    def fill_columns():
        for load in column_at:
            load.wait()
        cosines, sines = [], []
        for i in range(count // 8):
            cosine, sine = turned(column_coarse, column_fine, ((), ()), i)
            cosines.append(cosine.astype(bf16))
            sines.append((-sine).astype(bf16))
            slope_buf[8 * i : 8 * i + 8] = jnp.broadcast_to(sine[:, 1:2], (8, LANES))
        for i in range(0, count // 8, 2):
            column_buf[8 * i : 8 * i + 16] = jnp.concatenate(cosines[i : i + 2], axis=0)
            column_buf[count + 8 * i : count + 8 * i + 16] = jnp.concatenate(sines[i : i + 2], axis=0)

    def fill_rows():
        for load in row_at:
            load.wait()
        forward_coarse, forward_fine, backward_coarse, backward_fine = row_bufs
        for residue in range(4):
            for i in range(0, quarter // 8, 2):
                span = slice(8 * i, 8 * i + 16)
                for buf, coarse, fine, lead in (
                    (forward_buf, forward_coarse, forward_fine, ((residue,), (residue,))),
                    (backward_buf, backward_coarse, backward_fine, ((), (residue,))),
                ):
                    one, two = turned(coarse, fine, lead, i), turned(coarse, fine, lead, i + 1)
                    for part in range(2):
                        both = jnp.concatenate([one[part], two[part]], axis=0).astype(bf16)
                        buf[residue, span, quarter * part : quarter * (part + 1)] = both

    side = 16
    nodes = lax.broadcasted_iota(jnp.int32, (side, LANES), 0).astype(jnp.float32)

    def hats(place, tile):
        place = place[tile : tile + 1, :]
        cell = jnp.floor(place)
        high = place - cell
        block = jnp.floor(cell * (1.0 / side))
        node = cell - side * block
        here = jnp.where(nodes == node, 1.0 - high, jnp.where(nodes == node + 1.0, high, 0.0)).astype(bf16)
        following = jnp.where(nodes == node - (side - 1.0), high, 0.0).astype(bf16)
        number = jnp.broadcast_to(block, (side, LANES)).astype(bf16)
        none = jnp.zeros((side, LANES), bf16)
        before, blocks = None, []
        for k in range(extent // side):
            mine = number == jnp.asarray(k, bf16)
            rest = none if before is None else jnp.where(before, following, none)
            blocks.append(jnp.where(mine, here, rest))
            before = mine
        return jnp.concatenate(blocks, axis=0)

    def hat_pair(place, pair):
        return jnp.concatenate([hats(place, 2 * pair), hats(place, 2 * pair + 1)], axis=1)

    def column_sums(b):
        for pair in range(tiles // 2):
            span = slice(2 * LANES * pair, 2 * LANES * (pair + 1))
            found = dot(column_buf[...], hat_pair(position[b][1], pair))
            sums[b, :, span] = found
            heavy = jnp.concatenate([charge[b][2 * pair : 2 * pair + 1], charge[b][2 * pair + 1 : 2 * pair + 2]], axis=1)
            charged[b, :, span] = (found * heavy).astype(bf16)
            weight_rows[b, :, span] = hat_pair(position[b][0], pair)

    def column_spectrum(b):
        grid_spec[...] = dot_t(charged[b], weight_rows[b])

    side_rows = 16
    row_blocks = [slice(side_rows * i, side_rows * (i + 1)) for i in range(count // side_rows)]

    def imag_rows(rows):
        return slice(count + rows.start, count + rows.stop)

    def to_rows(residue):
        product[residue] = dot(turned_spec[residue], forward_buf[residue])

    def row_spectrum(residue, rows):
        below = imag_rows(rows)
        real = product[residue, rows, :quarter] + product[residue, below, quarter:]
        imag = product[residue, below, :quarter] - product[residue, rows, quarter:]
        return real, imag

    def kernel_spectrum():
        for load in green_at:
            load.wait()
        near[...] = dot_t(column_buf[...], green_buf[0].astype(bf16))
        far[...] = dot_t(column_buf[...], green_buf[1].astype(bf16))
        sign = (1 - 2 * lax.rem(rank, 2)).astype(jnp.float32)
        for rows in row_blocks:
            below = imag_rows(rows)
            re = [near[rows, quarter * m : quarter * (m + 1)] - sign * far[below, quarter * m : quarter * (m + 1)] for m in range(4)]
            im = [near[below, quarter * m : quarter * (m + 1)] + sign * far[rows, quarter * m : quarter * (m + 1)] for m in range(4)]
            even_re, odd_re, even_im, odd_im = re[0] + re[2], re[1] + re[3], im[0] + im[2], im[1] + im[3]
            far_re, turn_re, far_im, turn_im = re[0] - re[2], re[1] - re[3], im[0] - im[2], im[1] - im[3]
            put_turned(
                rows,
                (
                    (even_re + odd_re, even_im + odd_im),
                    (far_re + turn_im, far_im - turn_re),
                    (even_re - odd_re, even_im - odd_im),
                    (far_re - turn_im, far_im + turn_re),
                ),
            )
        scale = 2.0 / (period * period)
        for residue in range(4):
            to_rows(residue)
        for residue in range(4):
            for rows in row_blocks:
                real, imag = row_spectrum(residue, rows)
                spectrum_re[residue, rows] = real * scale
                spectrum_im[residue, rows] = imag * scale

    def put_turned(rows, turns_of):
        for residue, (re, im) in enumerate(turns_of):
            turned_spec[residue, rows] = re.astype(bf16)
            turned_spec[residue, imag_rows(rows)] = im.astype(bf16)

    def field_spectra():
        for rows in row_blocks:
            below = imag_rows(rows)
            re = grid_spec[rows, :quarter], grid_spec[rows, quarter:]
            im = grid_spec[below, :quarter], grid_spec[below, quarter:]
            put_turned(
                rows,
                (
                    (re[0] + re[1], im[0] + im[1]),
                    (re[0] + im[1], im[0] - re[1]),
                    (re[0] - re[1], im[0] - im[1]),
                    (re[0] - im[1], im[0] + re[1]),
                ),
            )
        to_rows(0)
        for residue in range(4):
            if residue + 1 < 4:
                to_rows(residue + 1)
            for rows in row_blocks:
                x_re, x_im = row_spectrum(residue, rows)
                k_re, k_im = spectrum_re[residue, rows], spectrum_im[residue, rows]
                scaled[residue, rows] = (x_re * k_re - x_im * k_im).astype(bf16)
                scaled[residue, imag_rows(rows)] = (x_re * k_im + x_im * k_re).astype(bf16)
            returned[residue] = dot(scaled[residue], backward_buf[residue])
        for rows in row_blocks:
            below = imag_rows(rows)
            for part in range(quarter // LANES):
                near_lanes = slice(LANES * part, LANES * (part + 1))
                far_lanes = slice(quarter + LANES * part, quarter + LANES * (part + 1))
                (a_re, a_im), (b_re, b_im), (c_re, c_im), (d_re, d_im) = [
                    (
                        returned[j, rows, near_lanes] - returned[j, below, far_lanes],
                        returned[j, below, near_lanes] + returned[j, rows, far_lanes],
                    )
                    for j in range(4)
                ]
                grid_spec[rows, near_lanes] = (a_re + c_re) + (b_re + d_re)
                grid_spec[below, near_lanes] = (a_im + c_im) + (b_im + d_im)
                grid_spec[rows, far_lanes] = (a_re - c_re) - (b_im - d_im)
                grid_spec[below, far_lanes] = (a_im - c_im) + (b_re - d_re)
        for rows in row_blocks:
            below = imag_rows(rows)
            slope = jnp.concatenate([slope_buf[rows]] * (extent // LANES), axis=1)
            for lines, twin, factor in ((rows, below, -slope), (below, rows, slope)):
                v = grid_spec[lines]
                fields[lines] = (0.5 * (pltpu.roll(v, 1, 1) - pltpu.roll(v, extent - 1, 1))).astype(bf16)
                fields[slice(2 * count + twin.start, 2 * count + twin.stop)] = (factor * v).astype(bf16)
        return fields[...]

    def kicks_on(b, spectra):
        rows = [[], []]
        for pair in range(tiles // 2):
            span = slice(2 * LANES * pair, 2 * LANES * (pair + 1))
            reached = dot(spectra, weight_rows[b, :, span])
            own = sums[b, :, span]
            for d in range(2):
                terms = reached[2 * count * d : 2 * count * (d + 1)] * own
                total = jnp.sum(jnp.sum(terms.reshape(2 * count // 8, 8, 2 * LANES), axis=0), axis=0, keepdims=True)
                rows[d] += [total[:, :LANES], total[:, LANES:]]
        return [jnp.concatenate(rows[d], axis=0) for d in range(2)]

    def send_kicks(section, b, parts):
        own = jnp.concatenate(parts, axis=0).astype(bf16)
        kick_src[section, b] = own
        for step in range(1 if b == 0 else 0, GROUP):
            copy = kick_copy(section, b, step)
            copy.start()
            sends.append(copy)
        return own

    def whole_momenta(b):
        for step in range(1 if b == 0 else 0, planes):
            momenta_copy(b, step).wait_recv()
        if b == 0:
            momenta_all[0, 0] = momenta_ref[0]
        result = []
        for d in range(2):
            each = []
            for plane in range(planes):
                slot = lax.rem(t - plane + planes, planes)
                each.append(momenta_all[b, slot, 0, d][None])
            share = LANES // width
            rows = [each[i] if share == 1 else jnp.concatenate(each[share * i : share * (i + 1)], axis=1) for i in range(tiles)]
            result.append(jnp.concatenate(rows, axis=0))
        return result

    def pass_on(section, parts):
        for i, part in enumerate(parts):
            forward_src[section, i] = part
        copy = forward_copy(section)
        copy.start()
        sends.append(copy)

    def arrive(section, b, own):
        if b == 0:
            if section == 0:
                momentum[0] = whole_momenta(0)
            old = [position[0][d] + DRIFT * momentum[0][d] for d in range(2)]
        else:
            forward_copy(section).wait_recv()
            old = [forward_dst[section, d] for d in range(2)]
            charge[1] = forward_dst[section, 4]
            if section == 0:
                momentum[1] = whole_momenta(1)
                old = [old[d] + DRIFT * momentum[1][d] for d in range(2)]
            else:
                momentum[1] = [forward_dst[section, 2 + d] for d in range(2)]
        total = own.astype(jnp.float32) if b == 0 else None
        for step in range(1 if b == 0 else 0, GROUP):
            kick_copy(section, b, step).wait_recv()
            part = kick_dst[section, b, step].astype(jnp.float32)
            total = part if total is None else total + part
        for d in range(2):
            kick = total[tiles * d : tiles * (d + 1)]
            momentum[b][d] = momentum[b][d] + kick
            position[b][d] = jnp.clip(old[d] + DRIFT * kick, 1.0, extent - 2.0 - 1.0 / 64.0)
        if b == 1 and section + 1 < SECTIONS - 1:
            pass_on(section + 1, [position[1][d] + DRIFT * momentum[1][d] for d in range(2)] + momentum[1] + [charge[1]])

    def send_last_kicks(b, parts):
        for i in range(tiles):
            rows = [parts[d][i : i + 1] for d in range(2)]
            last_src[b, i] = jnp.concatenate(rows + [jnp.zeros((6, LANES), jnp.float32)], axis=0)
        for step in range(1 if b == 0 else 0, GROUP):
            copy = last_copy(b, step)
            copy.start()
            sends.append(copy)

    def own_lanes(tile):
        share = LANES // width
        if share == 1:
            return tile
        place = lax.rem(t, share)
        result = tile[:, :width]
        for i in range(1, share):
            result = jnp.where(place == i, tile[:, width * i : width * (i + 1)], result)
        return result

    fill_columns()
    own_kicks = [None, None]
    first = 1
    for section in range(SECTIONS):
        second = 1 - first
        if section > 0:
            arrive(section - 1, first, own_kicks[first])
        column_sums(first)
        column_spectrum(first)
        if section == 0:
            fill_rows()
            kernel_spectrum()
        spectra = field_spectra()
        if section > 0:
            arrive(section - 1, second, own_kicks[second])
        column_sums(second)
        for source, target in ((first, second), (second, first)):
            if source == second:
                column_spectrum(second)
                spectra = field_spectra()
            parts = kicks_on(target, spectra)
            if section == 0 and source == first:
                pl.semaphore_wait(barrier, greeted)
                copies = [momenta_copy(b, step) for b in range(2) for step in range(1 - b, planes)]
                for copy in copies:
                    copy.start()
                sends += copies
                pass_on(0, position[1] + [jnp.zeros_like(charge[1])] * 2 + [charge[1]])
            if section + 1 < SECTIONS:
                own_kicks[target] = send_kicks(section, target, parts)
            else:
                share = 1.0 / GROUP
                send_last_kicks(target, [parts[d] + share * momentum[target][d] for d in range(2)])
        first = second

    for b in (1, 0):
        total = last_src[0, (t * width) // LANES] if b == 0 else None
        for step in range(1 if b == 0 else 0, GROUP):
            last_copy(b, step).wait_recv()
            total = last_dst[b, step] if total is None else total + last_dst[b, step]
        out_ref[b, 0] = own_lanes(total[0:2])
    for copy in sends:
        copy.wait_send()


def per_device(mesh_shape, cells, offsets, charges, momenta, green):
    columns, planes = mesh_shape
    period = green.shape[0]
    extent = period // 2
    quarter = period // 4
    particles = cells.shape[-1]
    tiles = particles // LANES
    count = extent // GROUP
    tables = column_tables(period) + row_tables(period)
    vmem = pl.BlockSpec(memory_space=pltpu.VMEM)
    anywhere = pl.BlockSpec(memory_space=pl.ANY)
    dma = pltpu.SemaphoreType.DMA
    f32, bf16 = jnp.float32, jnp.bfloat16
    return pl.pallas_call(
        functools.partial(kernel, (columns, planes, extent, particles)),
        out_shape=jax.ShapeDtypeStruct(momenta.shape, momenta.dtype),
        in_specs=[vmem] * 4 + [anywhere] * 7,
        out_specs=vmem,
        scratch_shapes=[
            pltpu.VMEM(tables[0].shape, f32),
            pltpu.VMEM(tables[1].shape[1:], f32),
            *[pltpu.VMEM(table.shape, f32) for table in tables[2:]],
            pltpu.VMEM((2, period, extent), f32),
            pltpu.VMEM((2 * count, extent), bf16),
            pltpu.VMEM((count, LANES), f32),
            pltpu.VMEM((4, quarter, 2 * quarter), bf16),
            pltpu.VMEM((4, quarter, 2 * quarter), bf16),
            pltpu.VMEM((4, count, quarter), f32),
            pltpu.VMEM((4, count, quarter), f32),
            pltpu.VMEM((2, 2 * count, particles), f32),
            pltpu.VMEM((2, 2 * count, particles), bf16),
            pltpu.VMEM((2, extent, particles), bf16),
            pltpu.VMEM((2 * count, extent), f32),
            pltpu.VMEM((4, 2 * count, quarter), bf16),
            pltpu.VMEM((4, 2 * count, 2 * quarter), f32),
            pltpu.VMEM((4, 2 * count, quarter), bf16),
            pltpu.VMEM((4, 2 * count, 2 * quarter), f32),
            pltpu.VMEM((4 * count, extent), bf16),
            pltpu.VMEM((2 * count, period), f32),
            pltpu.VMEM((2 * count, period), f32),
            pltpu.VMEM((2, planes, *momenta.shape[1:]), f32),
            pltpu.VMEM((SECTIONS - 1, 5, tiles, LANES), f32),
            pltpu.VMEM((SECTIONS - 1, 5, tiles, LANES), f32),
            pltpu.VMEM((SECTIONS - 1, 2, 2 * tiles, LANES), bf16),
            pltpu.VMEM((SECTIONS - 1, 2, GROUP, 2 * tiles, LANES), bf16),
            pltpu.VMEM((2, tiles, 8, LANES), f32),
            pltpu.VMEM((2, GROUP, 8, LANES), f32),
            dma((8,)),
            dma((2, planes)),
            dma((2, planes)),
            dma((SECTIONS - 1,)),
            dma((SECTIONS - 1,)),
            dma((SECTIONS - 1, 2, GROUP)),
            dma((SECTIONS - 1, 2, GROUP)),
            dma((2, GROUP)),
            dma((2, GROUP)),
        ],
        compiler_params=pltpu.CompilerParams(collective_id=0, has_side_effects=True, vmem_limit_bytes=60 * 1024 * 1024),
    )(cells, offsets, charges, momenta, green, *tables)


def solution(mesh):
    return jax.shard_map(
        functools.partial(per_device, (mesh.shape["cuts"], mesh.shape["tr"])),
        mesh=mesh,
        in_specs=(
            P(None, "cuts", None, None),
            P(None, "cuts", None, None),
            P(None, "cuts", None),
            P(None, "cuts", None, "tr"),
            P(),
        ),
        out_specs=P(None, "cuts", None, "tr"),
        check_vma=False,
    )
```

```python
import functools
import math

import jax
import jax.numpy as jnp
import numpy as np
from jax import lax
from jax.experimental import pallas as pl
from jax.experimental.pallas import tpu as pltpu
from jax.sharding import PartitionSpec as P

SECTIONS = 4
GROUP = 4
LANES = 128
DRIFT = 0.5
MESH = pl.DeviceIdType.MESH


def turns(angle_steps, period):
    angle = 2.0 * np.pi / period * (angle_steps % period)
    return np.stack([np.cos(angle), np.sin(angle)], axis=-3).astype(np.float32)


def row_tables(period):
    near = np.arange(period // 4)
    coarse, fine = np.arange(period // 32), np.arange(8)
    residue = np.arange(4)[:, None, None]
    frequency = 4 * near[None, None, :] + residue
    forward_coarse = turns(8 * coarse[None, :, None] * frequency, period)
    forward_fine = turns(fine[None, :, None] * frequency, period)
    backward_coarse = turns(32 * coarse[:, None] * near[None, :], period)
    backward_fine = turns((4 * fine[None, :, None] + residue) * near[None, None, :], period)
    return forward_coarse, forward_fine, backward_coarse, backward_fine


def column_tables(period):
    column = np.arange(period // 2)
    coarse = np.arange(period // 2 // GROUP // 8)
    fine = 2 * (GROUP * np.arange(8)[None, :] + np.arange(GROUP)[:, None]) + 1
    return turns(8 * GROUP * coarse[:, None] * column[None, :], period), turns(fine[:, :, None] * column, 2 * period)


def dot(left, right):
    return lax.dot_general(left, right, (((1,), (0,)), ((), ())), preferred_element_type=jnp.float32)


def dot_t(left, right):
    return lax.dot_general(left, right, (((1,), (1,)), ((), ())), preferred_element_type=jnp.float32)


def kernel(
    sizes,
    cells_ref, offsets_ref, charges_ref, momenta_ref, green_ref, column_hbm, column_fine_hbm, *row_hbm_and_rest,
):
    row_hbm = row_hbm_and_rest[:4]
    (

    out_ref, column_coarse, column_fine, *row_bufs_and_rest) = row_hbm_and_rest[4:]
    row_bufs = row_bufs_and_rest[:4]
    (green_buf, column_buf, slope_buf, forward_buf, backward_buf, spectrum_re, spectrum_im,
    sums, charged, weight_rows, grid_spec, turned_spec, product, scaled, returned, fields, near, far, momenta_all, forward_src, forward_dst, kick_src, kick_dst, last_src, last_dst,
    load_sem, fence_sem, send_mom, recv_mom, send_fwd, recv_fwd, send_kick, recv_kick, send_last, recv_last) = row_bufs_and_rest[4:]
    columns, planes, extent, particles = sizes
    period = 2 * extent
    quarter = period // 4
    count = extent // GROUP
    tiles = particles // LANES
    width = particles // planes
    bf16 = jnp.bfloat16

    c = lax.axis_index("cuts")
    t = lax.axis_index("tr")
    rank = lax.rem(t, GROUP)
    base = t - rank
    ahead = lax.rem(c + columns - 2, columns)
    behind = lax.rem(c + 2, columns)
    home = lax.rem(c + 2 * (SECTIONS - 1), columns)
    origin = lax.rem(c + columns - 2 * (SECTIONS - 1), columns)

    def member(step):
        return base + lax.rem(rank + step, GROUP)

    green_at = [pltpu.make_async_copy(green_ref.at[:, pl.ds(h * extent, extent)], green_buf.at[h], load_sem.at[h]) for h in range(2)]
    column_at = [
        pltpu.make_async_copy(column_hbm, column_coarse, load_sem.at[2]),
        pltpu.make_async_copy(column_fine_hbm.at[rank], column_fine, load_sem.at[3]),
    ]
    row_at = [pltpu.make_async_copy(row_hbm[i], row_bufs[i], load_sem.at[4 + i]) for i in range(4)]
    for load in column_at + green_at + row_at:
        load.start()

    barrier = pltpu.get_barrier_semaphore()

    def greet(column, plane):
        pl.semaphore_signal(barrier, inc=1, device_id={"cuts": column, "tr": plane}, device_id_type=MESH)

    for step in range(1, planes):
        greet(c, lax.rem(t + step, planes))
    for step in range(planes):
        greet(ahead, lax.rem(t + step, planes))
        greet(behind, lax.rem(t + step, planes))
    for step in range(GROUP):
        greet(home, member(step))
        greet(origin, member(step))
    greeted = planes - 1 + 2 * planes + 2 * GROUP

    def packed(ref, lead):
        return jnp.concatenate([ref[lead + (slice(LANES * i, LANES * (i + 1)),)][None] for i in range(tiles)], axis=0)

    position = [
        [packed(cells_ref, (b, 0, d)).astype(jnp.float32) + packed(offsets_ref, (b, 0, d)) for d in range(2)] for b in range(2)
    ]
    charge = [packed(charges_ref, (b, 0)) for b in range(2)]
    momentum = [[None, None], [None, None]]

    def copy_to(source, target, send, receive, column, plane):
        return pltpu.make_async_remote_copy(
            src_ref=source, dst_ref=target, send_sem=send, recv_sem=receive,
            device_id={"cuts": column, "tr": plane}, device_id_type=MESH,
        )

    sends = []

    def forward_copy(section):
        return copy_to(forward_src.at[section], forward_dst.at[section], send_fwd.at[section], recv_fwd.at[section], ahead, t)

    def momenta_copy(b, step):
        column = c if b == 0 else ahead
        return copy_to(
            momenta_ref.at[b], momenta_all.at[b, step], send_mom.at[b, step], recv_mom.at[b, step], column, lax.rem(t + step, planes)
        )

    def kick_copy(section, b, step):
        column = c if b == 0 else ahead
        return copy_to(
            kick_src.at[section, b], kick_dst.at[section, b, step], send_kick.at[section, b, step], recv_kick.at[section, b, step],
            column, member(step),
        )

    def last_copy(b, step):
        column = c if b == 0 else home
        plane = member(step)
        return copy_to(
            last_src.at[b, (plane * width) // LANES], last_dst.at[b, step], send_last.at[b, step], recv_last.at[b, step], column, plane
        )

    def turned(coarse_ref, fine_ref, lead, first):
        far_cos, far_sin = coarse_ref[lead[0] + (0, slice(first, first + 1))], coarse_ref[lead[0] + (1, slice(first, first + 1))]
        near_cos, near_sin = fine_ref[lead[1] + (0,)], fine_ref[lead[1] + (1,)]
        return far_cos * near_cos - far_sin * near_sin, far_sin * near_cos + far_cos * near_sin

    def fill_columns():
        for load in column_at:
            load.wait()
        cosines, sines = [], []
        for i in range(count // 8):
            cosine, sine = turned(column_coarse, column_fine, ((), ()), i)
            cosines.append(cosine.astype(bf16))
            sines.append((-sine).astype(bf16))
            slope_buf[8 * i : 8 * i + 8] = jnp.broadcast_to(sine[:, 1:2], (8, LANES))
        for i in range(0, count // 8, 2):
            column_buf[8 * i : 8 * i + 16] = jnp.concatenate(cosines[i : i + 2], axis=0)
            column_buf[count + 8 * i : count + 8 * i + 16] = jnp.concatenate(sines[i : i + 2], axis=0)

    def fill_rows():
        for load in row_at:
            load.wait()
        forward_coarse, forward_fine, backward_coarse, backward_fine = row_bufs
        for residue in range(4):
            for i in range(0, quarter // 8, 2):
                span = slice(8 * i, 8 * i + 16)
                for buf, coarse, fine, lead in (
                    (forward_buf, forward_coarse, forward_fine, ((residue,), (residue,))),
                    (backward_buf, backward_coarse, backward_fine, ((), (residue,))),
                ):
                    one, two = turned(coarse, fine, lead, i), turned(coarse, fine, lead, i + 1)
                    for part in range(2):
                        both = jnp.concatenate([one[part], two[part]], axis=0).astype(bf16)
                        buf[residue, span, quarter * part : quarter * (part + 1)] = both

    side = 16
    nodes = lax.broadcasted_iota(jnp.int32, (side, LANES), 0).astype(jnp.float32)

    def hats(place, tile):
        place = place[tile : tile + 1, :]
        cell = jnp.floor(place)
        high = place - cell
        block = jnp.floor(cell * (1.0 / side))
        node = cell - side * block
        here = jnp.where(nodes == node, 1.0 - high, jnp.where(nodes == node + 1.0, high, 0.0)).astype(bf16)
        following = jnp.where(nodes == node - (side - 1.0), high, 0.0).astype(bf16)
        number = jnp.broadcast_to(block, (side, LANES)).astype(bf16)
        none = jnp.zeros((side, LANES), bf16)
        before, blocks = None, []
        for k in range(extent // side):
            mine = number == jnp.asarray(k, bf16)
            rest = none if before is None else jnp.where(before, following, none)
            blocks.append(jnp.where(mine, here, rest))
            before = mine
        return jnp.concatenate(blocks, axis=0)

    def hat_pair(place, pair):
        return jnp.concatenate([hats(place, 2 * pair), hats(place, 2 * pair + 1)], axis=1)

    def column_sums(b):
        for pair in range(tiles // 2):
            span = slice(2 * LANES * pair, 2 * LANES * (pair + 1))
            found = dot(column_buf[...], hat_pair(position[b][1], pair))
            sums[b, :, span] = found
            heavy = jnp.concatenate([charge[b][2 * pair : 2 * pair + 1], charge[b][2 * pair + 1 : 2 * pair + 2]], axis=1)
            charged[b, :, span] = (found * heavy).astype(bf16)
            weight_rows[b, :, span] = hat_pair(position[b][0], pair)

    def column_spectrum(b):
        grid_spec[...] = dot_t(charged[b], weight_rows[b])

    side_rows = 16
    row_blocks = [slice(side_rows * i, side_rows * (i + 1)) for i in range(count // side_rows)]

    def imag_rows(rows):
        return slice(count + rows.start, count + rows.stop)

    def to_rows(residue):
        product[residue] = dot(turned_spec[residue], forward_buf[residue])

    def row_spectrum(residue, rows):
        below = imag_rows(rows)
        real = product[residue, rows, :quarter] + product[residue, below, quarter:]
        imag = product[residue, below, :quarter] - product[residue, rows, quarter:]
        return real, imag

    def kernel_spectrum():
        for load in green_at:
            load.wait()
        near[...] = dot_t(column_buf[...], green_buf[0].astype(bf16))
        far[...] = dot_t(column_buf[...], green_buf[1].astype(bf16))
        sign = (1 - 2 * lax.rem(rank, 2)).astype(jnp.float32)
        for rows in row_blocks:
            below = imag_rows(rows)
            re = [near[rows, quarter * m : quarter * (m + 1)] - sign * far[below, quarter * m : quarter * (m + 1)] for m in range(4)]
            im = [near[below, quarter * m : quarter * (m + 1)] + sign * far[rows, quarter * m : quarter * (m + 1)] for m in range(4)]
            even_re, odd_re, even_im, odd_im = re[0] + re[2], re[1] + re[3], im[0] + im[2], im[1] + im[3]
            far_re, turn_re, far_im, turn_im = re[0] - re[2], re[1] - re[3], im[0] - im[2], im[1] - im[3]
            put_turned(
                rows,
                (
                    (even_re + odd_re, even_im + odd_im),
                    (far_re + turn_im, far_im - turn_re),
                    (even_re - odd_re, even_im - odd_im),
                    (far_re - turn_im, far_im + turn_re),
                ),
            )
        scale = 2.0 / (period * period)
        for residue in range(4):
            to_rows(residue)
        for residue in range(4):
            for rows in row_blocks:
                real, imag = row_spectrum(residue, rows)
                spectrum_re[residue, rows] = real * scale
                spectrum_im[residue, rows] = imag * scale

    def put_turned(rows, turns_of):
        for residue, (re, im) in enumerate(turns_of):
            turned_spec[residue, rows] = re.astype(bf16)
            turned_spec[residue, imag_rows(rows)] = im.astype(bf16)

    def field_spectra():
        for rows in row_blocks:
            below = imag_rows(rows)
            re = grid_spec[rows, :quarter], grid_spec[rows, quarter:]
            im = grid_spec[below, :quarter], grid_spec[below, quarter:]
            put_turned(
                rows,
                (
                    (re[0] + re[1], im[0] + im[1]),
                    (re[0] + im[1], im[0] - re[1]),
                    (re[0] - re[1], im[0] - im[1]),
                    (re[0] - im[1], im[0] + re[1]),
                ),
            )
        to_rows(0)
        for residue in range(4):
            if residue + 1 < 4:
                to_rows(residue + 1)
            for rows in row_blocks:
                x_re, x_im = row_spectrum(residue, rows)
                k_re, k_im = spectrum_re[residue, rows], spectrum_im[residue, rows]
                scaled[residue, rows] = (x_re * k_re - x_im * k_im).astype(bf16)
                scaled[residue, imag_rows(rows)] = (x_re * k_im + x_im * k_re).astype(bf16)
            returned[residue] = dot(scaled[residue], backward_buf[residue])
        for rows in row_blocks:
            below = imag_rows(rows)
            for part in range(quarter // LANES):
                near_lanes = slice(LANES * part, LANES * (part + 1))
                far_lanes = slice(quarter + LANES * part, quarter + LANES * (part + 1))
                (a_re, a_im), (b_re, b_im), (c_re, c_im), (d_re, d_im) = [
                    (
                        returned[j, rows, near_lanes] - returned[j, below, far_lanes],
                        returned[j, below, near_lanes] + returned[j, rows, far_lanes],
                    )
                    for j in range(4)
                ]
                grid_spec[rows, near_lanes] = (a_re + c_re) + (b_re + d_re)
                grid_spec[below, near_lanes] = (a_im + c_im) + (b_im + d_im)
                grid_spec[rows, far_lanes] = (a_re - c_re) - (b_im - d_im)
                grid_spec[below, far_lanes] = (a_im - c_im) + (b_re - d_re)
        for rows in row_blocks:
            below = imag_rows(rows)
            slope = jnp.concatenate([slope_buf[rows]] * (extent // LANES), axis=1)
            for lines, twin, factor in ((rows, below, -slope), (below, rows, slope)):
                v = grid_spec[lines]
                fields[lines] = (0.5 * (pltpu.roll(v, 1, 1) - pltpu.roll(v, extent - 1, 1))).astype(bf16)
                fields[slice(2 * count + twin.start, 2 * count + twin.stop)] = (factor * v).astype(bf16)
        return fields[...]

    def kicks_on(b, spectra):
        rows = [[], []]
        for pair in range(tiles // 2):
            span = slice(2 * LANES * pair, 2 * LANES * (pair + 1))
            reached = dot(spectra, weight_rows[b, :, span])
            own = sums[b, :, span]
            for d in range(2):
                terms = reached[2 * count * d : 2 * count * (d + 1)] * own
                total = jnp.sum(jnp.sum(terms.reshape(2 * count // 8, 8, 2 * LANES), axis=0), axis=0, keepdims=True)
                rows[d] += [total[:, :LANES], total[:, LANES:]]
        return [jnp.concatenate(rows[d], axis=0) for d in range(2)]

    def fence():
        pl.semaphore_signal(fence_sem, 1)
        pl.semaphore_wait(fence_sem, 1)

    def send_kicks(section, b, parts):
        own = jnp.concatenate(parts, axis=0).astype(bf16)
        kick_src[section, b] = own
        for step in range(1 if b == 0 else 0, GROUP):
            copy = kick_copy(section, b, step)
            copy.start()
            sends.append(copy)
        return own

    def whole_momenta(b):
        for step in range(1 if b == 0 else 0, planes):
            momenta_copy(b, step).wait_recv()
        if b == 0:
            momenta_all[0, 0] = momenta_ref[0]
        result = []
        for d in range(2):
            each = []
            for plane in range(planes):
                slot = lax.rem(t - plane + planes, planes)
                each.append(momenta_all[b, slot, 0, d][None])
            share = LANES // width
            rows = [each[i] if share == 1 else jnp.concatenate(each[share * i : share * (i + 1)], axis=1) for i in range(tiles)]
            result.append(jnp.concatenate(rows, axis=0))
        return result

    def pass_on(section, parts):
        for i, part in enumerate(parts):
            forward_src[section, i] = part
        copy = forward_copy(section)
        copy.start()
        sends.append(copy)

    def arrive(section, b, own):
        if b == 0:
            if section == 0:
                momentum[0] = whole_momenta(0)
            old = [position[0][d] + DRIFT * momentum[0][d] for d in range(2)]
        else:
            forward_copy(section).wait_recv()
            old = [forward_dst[section, d] for d in range(2)]
            charge[1] = forward_dst[section, 4]
            if section == 0:
                momentum[1] = whole_momenta(1)
                old = [old[d] + DRIFT * momentum[1][d] for d in range(2)]
            else:
                momentum[1] = [forward_dst[section, 2 + d] for d in range(2)]
        total = own.astype(jnp.float32) if b == 0 else None
        for step in range(1 if b == 0 else 0, GROUP):
            kick_copy(section, b, step).wait_recv()
            part = kick_dst[section, b, step].astype(jnp.float32)
            total = part if total is None else total + part
        for d in range(2):
            kick = total[tiles * d : tiles * (d + 1)]
            momentum[b][d] = momentum[b][d] + kick
            position[b][d] = jnp.clip(old[d] + DRIFT * kick, 1.0, extent - 2.0 - 1.0 / 64.0)
        if b == 1 and section + 1 < SECTIONS - 1:
            pass_on(section + 1, [position[1][d] + DRIFT * momentum[1][d] for d in range(2)] + momentum[1] + [charge[1]])

    def send_last_kicks(b, parts):
        for i in range(tiles):
            rows = [parts[d][i : i + 1] for d in range(2)]
            last_src[b, i] = jnp.concatenate(rows + [jnp.zeros((6, LANES), jnp.float32)], axis=0)
        for step in range(1 if b == 0 else 0, GROUP):
            copy = last_copy(b, step)
            copy.start()
            sends.append(copy)

    def own_lanes(tile):
        share = LANES // width
        if share == 1:
            return tile
        place = lax.rem(t, share)
        result = tile[:, :width]
        for i in range(1, share):
            result = jnp.where(place == i, tile[:, width * i : width * (i + 1)], result)
        return result

    fill_columns()
    own_kicks = [None, None]
    first = 1
    for section in range(SECTIONS):
        second = 1 - first
        if section > 0:
            arrive(section - 1, first, own_kicks[first])
        column_sums(first)
        column_spectrum(first)
        if section == 0:
            fill_rows()
            kernel_spectrum()
        spectra = field_spectra()
        if section > 0:
            arrive(section - 1, second, own_kicks[second])
        column_sums(second)
        for source, target in ((first, second), (second, first)):
            if source == second:
                column_spectrum(second)
                spectra = field_spectra()
            parts = kicks_on(target, spectra)
            if section == 0 and source == first:
                pl.semaphore_wait(barrier, greeted)
                copies = [momenta_copy(b, step) for b in range(2) for step in range(1 - b, planes)]
                for copy in copies:
                    copy.start()
                sends += copies
                pass_on(0, position[1] + [jnp.zeros_like(charge[1])] * 2 + [charge[1]])
            if section + 1 < SECTIONS:
                own_kicks[target] = send_kicks(section, target, parts)
            else:
                share = 1.0 / GROUP
                send_last_kicks(target, [parts[d] + share * momentum[target][d] for d in range(2)])
            if source == first:
                fence()
        first = second

    for b in (1, 0):
        total = last_src[0, (t * width) // LANES] if b == 0 else None
        for step in range(1 if b == 0 else 0, GROUP):
            last_copy(b, step).wait_recv()
            total = last_dst[b, step] if total is None else total + last_dst[b, step]
        out_ref[b, 0] = own_lanes(total[0:2])
    for copy in sends:
        copy.wait_send()


def per_device(mesh_shape, cells, offsets, charges, momenta, green):
    columns, planes = mesh_shape
    period = green.shape[0]
    extent = period // 2
    quarter = period // 4
    particles = cells.shape[-1]
    tiles = particles // LANES
    count = extent // GROUP
    tables = column_tables(period) + row_tables(period)
    vmem = pl.BlockSpec(memory_space=pltpu.VMEM)
    anywhere = pl.BlockSpec(memory_space=pl.ANY)
    dma = pltpu.SemaphoreType.DMA
    f32, bf16 = jnp.float32, jnp.bfloat16
    return pl.pallas_call(
        functools.partial(kernel, (columns, planes, extent, particles)),
        out_shape=jax.ShapeDtypeStruct(momenta.shape, momenta.dtype),
        in_specs=[vmem] * 4 + [anywhere] * 7,
        out_specs=vmem,
        scratch_shapes=[
            pltpu.VMEM(tables[0].shape, f32),
            pltpu.VMEM(tables[1].shape[1:], f32),
            *[pltpu.VMEM(table.shape, f32) for table in tables[2:]],
            pltpu.VMEM((2, period, extent), f32),
            pltpu.VMEM((2 * count, extent), bf16),
            pltpu.VMEM((count, LANES), f32),
            pltpu.VMEM((4, quarter, 2 * quarter), bf16),
            pltpu.VMEM((4, quarter, 2 * quarter), bf16),
            pltpu.VMEM((4, count, quarter), f32),
            pltpu.VMEM((4, count, quarter), f32),
            pltpu.VMEM((2, 2 * count, particles), f32),
            pltpu.VMEM((2, 2 * count, particles), bf16),
            pltpu.VMEM((2, extent, particles), bf16),
            pltpu.VMEM((2 * count, extent), f32),
            pltpu.VMEM((4, 2 * count, quarter), bf16),
            pltpu.VMEM((4, 2 * count, 2 * quarter), f32),
            pltpu.VMEM((4, 2 * count, quarter), bf16),
            pltpu.VMEM((4, 2 * count, 2 * quarter), f32),
            pltpu.VMEM((4 * count, extent), bf16),
            pltpu.VMEM((2 * count, period), f32),
            pltpu.VMEM((2 * count, period), f32),
            pltpu.VMEM((2, planes, *momenta.shape[1:]), f32),
            pltpu.VMEM((SECTIONS - 1, 5, tiles, LANES), f32),
            pltpu.VMEM((SECTIONS - 1, 5, tiles, LANES), f32),
            pltpu.VMEM((SECTIONS - 1, 2, 2 * tiles, LANES), bf16),
            pltpu.VMEM((SECTIONS - 1, 2, GROUP, 2 * tiles, LANES), bf16),
            pltpu.VMEM((2, tiles, 8, LANES), f32),
            pltpu.VMEM((2, GROUP, 8, LANES), f32),
            dma((8,)),
            pltpu.SemaphoreType.REGULAR,
            dma((2, planes)),
            dma((2, planes)),
            dma((SECTIONS - 1,)),
            dma((SECTIONS - 1,)),
            dma((SECTIONS - 1, 2, GROUP)),
            dma((SECTIONS - 1, 2, GROUP)),
            dma((2, GROUP)),
            dma((2, GROUP)),
        ],
        compiler_params=pltpu.CompilerParams(collective_id=0, has_side_effects=True, vmem_limit_bytes=60 * 1024 * 1024),
    )(cells, offsets, charges, momenta, green, *tables)


def solution(mesh):
    return jax.shard_map(
        functools.partial(per_device, (mesh.shape["cuts"], mesh.shape["tr"])),
        mesh=mesh,
        in_specs=(
            P(None, "cuts", None, None),
            P(None, "cuts", None, None),
            P(None, "cuts", None),
            P(None, "cuts", None, "tr"),
            P(),
        ),
        out_specs=P(None, "cuts", None, "tr"),
        check_vma=False,
    )
```
